128 devices in a mesh: dev: 128 (over z, x, y, core).
Axes of the slice: x: 4, y: 4, z: 4, core: 2. Of those that a mesh axis runs over, the one named last changes fastest.
Arguments:
- gradient: bfloat16 [65536, 1024], P('dev'), may hold values from -0.1875 to 0.1875
- statistics: float32 [128, 1024, 1024], P('dev')
- held_roots: bfloat16 [128, 1024, 1024], P('dev')
- pending_roots: bfloat16 [256, 1024, 1024], P('dev')
- pending_stat: int32 [256], replicated, may hold values from -1 to 127, as said below
- refresh_stat: int32 [256], replicated, may hold values from -1 to 127, as said below
Outputs:
- new_statistics: float32 [128, 1024, 1024], P('dev')
- merged_roots: bfloat16 [128, 1024, 1024], P('dev')
- direction: bfloat16 [65536, 1024], P('dev')
- fresh_roots: bfloat16 [256, 1024, 1024], P('dev')
The draws below stay inside these ranges and needn't reach their ends.
Inputs may be any that keep to these rules, and one draw needn't show every extreme that they name: `refresh_stat`: entry w * 2 + k is the slot k of device w. Exactly 64 entries are not -1, each naming a different statistic, and at least one device has all 2 of its slots used. `pending_stat`: entry w * 2 + k names the statistic whose root stands in pending_roots at that index. Exactly 64 entries are not -1, each naming a different statistic, and at least one device has all 2 of its slots used.
All inputs are finite; a program needn't handle non-finite values.
Results may differ from the reference program's by a relative error of at most 0.012.
Values may be sent and summed in bfloat16 or wider, within the bound.
No kernel may reach another device: no remote copies, remote signals or barrier semaphores. Data moves between devices by JAX's collectives and lax.ppermute only.
A program may use at most 128 MiB of HBM per device.

```python
import math
import jax
import jax.numpy as jnp
from jax import lax

B = 1024
SLOTS = 2
ITERS = 2
BLOCKS = 64
N_DEV = 128


def spd_blocks(key, block_count, block_width, lower_bound, upper_bound, spread):
    key_diag, key_noise = jax.random.split(key)
    scales = jnp.exp(jax.random.uniform(key_diag, (block_count, block_width), jnp.float32, math.log(lower_bound), math.log(upper_bound)))
    noise_part = jax.random.normal(key_noise, (block_count, block_width, block_width), jnp.float32) * (spread / math.sqrt(block_width))
    symmetric = (noise_part + jnp.swapaxes(noise_part, 1, 2)) / math.sqrt(2.0)
    identity = jnp.eye(block_width, dtype=jnp.float32)
    root_scales = jnp.sqrt(scales)
    return root_scales[:, :, None] * (identity[None] + symmetric) * root_scales[:, None, :]


def slot_assignment(key):
    total_slots = N_DEV * SLOTS
    chosen_total = N_DEV // 2
    key_stat, key_work, key_pair, key_side = jax.random.split(key, 4)
    stat_order = jax.random.permutation(key_stat, N_DEV)[:chosen_total]
    worker_order = jax.random.permutation(key_work, N_DEV)
    doubled = jax.random.randint(key_pair, (), 1, max(chosen_total // 4, 1) + 1)
    ranks = jnp.arange(chosen_total, dtype=jnp.int32)
    paired = ranks < 2 * doubled
    worker_pos = jnp.where(paired, ranks // 2, ranks - doubled)
    side_pick = jax.random.randint(key_side, (chosen_total,), 0, 2)
    slot_pos = jnp.where(paired, ranks % 2, side_pick)
    target = worker_order[worker_pos] * SLOTS + slot_pos
    return jnp.full((total_slots,), -1, jnp.int32).at[target].set(stat_order.astype(jnp.int32))


def draw_statistics(key, part):
    return spd_blocks(jax.random.fold_in(key, 7), N_DEV, B, 0.3, 3.0, 0.35)


def draw_held_roots(key, part):
    values = spd_blocks(jax.random.fold_in(key, 11), N_DEV, B, 0.5, 2.0, 0.35)
    return values.astype(jnp.bfloat16)


def draw_pending_roots(key, part):
    values = spd_blocks(jax.random.fold_in(key, 13), N_DEV * SLOTS, B, 0.5, 2.0, 0.35)
    return values.astype(jnp.bfloat16)


def draw_pending_stat(key, part):
    return slot_assignment(jax.random.fold_in(key, 5))


def draw_refresh_stat(key, part):
    return slot_assignment(jax.random.fold_in(key, 3))


def steps_of(key, shape, pieces, smallest, top_value):
    def one(axis_at, shards_of):
        heights = jax.random.uniform(jax.random.fold_in(jax.random.fold_in(key, 6), axis_at), (shards_of,), jnp.float32, smallest / len(pieces), top_value / len(pieces))
        return jnp.repeat(jnp.exp(heights), shape[axis_at] // shards_of).reshape((-1,) + (1,) * (len(shape) - axis_at - 1))

    gain = one(*pieces[0])
    for cut in pieces[1:]:
        gain = gain * one(*cut)
    return gain


def noise(rng, extent, deviation, reach, pieces=(), kind=jnp.bfloat16):
    drawn = deviation * jax.random.normal(rng, extent, jnp.float32)
    if pieces:
        drawn = drawn * steps_of(rng, extent, pieces, -0.22, 0.18)
    return jnp.clip(drawn, -reach, reach).astype(kind)


def setup_inputs(seed: int = 0) -> dict:
    keys = jax.random.split(jax.random.key(seed), 7)
    gradient = noise(keys[0], (BLOCKS * B, B), B ** -0.5, 0.1875, ((0, 128),))
    statistics = draw_statistics(jax.random.fold_in(keys[6], 71), 0)
    held_roots = draw_held_roots(jax.random.fold_in(keys[6], 71), 0)
    pending_roots = draw_pending_roots(jax.random.fold_in(keys[6], 71), 0)
    pending_stat = draw_pending_stat(jax.random.fold_in(keys[6], 71), 0)
    refresh_stat = draw_refresh_stat(jax.random.fold_in(keys[6], 71), 0)
    return dict(gradient=gradient, statistics=statistics, held_roots=held_roots, pending_roots=pending_roots, pending_stat=pending_stat, refresh_stat=refresh_stat)


decay_rate = 0.9

def poly_times(first, second):
    result = [0.0] * (len(first) + len(second) - 1)
    for left_pos in range(len(first)):
        for right_pos in range(len(second)):
            result[left_pos + right_pos] += first[left_pos] * second[right_pos]
    return result

def root_polynomial(iteration_count):
    x_poly = [1.0]
    m_poly = [0.0, 1.0]
    for newton_turn in range(iteration_count):
        t_poly = [-value / 4.0 for value in m_poly]
        t_poly[0] += 5.0 / 4.0
        x_poly = poly_times(x_poly, t_poly)
        t_square = poly_times(t_poly, t_poly)
        m_poly = poly_times(poly_times(t_square, t_square), m_poly)
    return [float(value) for value in x_poly]

def matmul_exact(first, second):
    return jnp.dot(first, second, precision=lax.Precision.HIGHEST, preferred_element_type=jnp.float32)

def inverse_root(statistic):
    size_b = statistic.shape[0]
    identity = jnp.eye(size_b, dtype=jnp.float32)
    norm_scale = 2.0 * jnp.trace(statistic) / size_b
    scaled = statistic / norm_scale
    coefficients = root_polynomial(ITERS)
    scaled_sq = matmul_exact(scaled, scaled)
    scaled_cube = matmul_exact(scaled_sq, scaled)
    lower_part = coefficients[0] * identity + coefficients[1] * scaled + coefficients[2] * scaled_sq
    upper_part = coefficients[3] * identity + coefficients[4] * scaled + coefficients[5] * scaled_sq + coefficients[6] * scaled_cube
    polynomial = lower_part + matmul_exact(scaled_cube, upper_part)
    return polynomial * norm_scale ** (-0.25)

def reference(gradient, statistics, held_roots, pending_roots, pending_stat, refresh_stat):
    stat_count = statistics.shape[0]
    block_width = statistics.shape[1]
    grads = gradient.reshape(stat_count // 2, block_width, block_width)

    def gram_pair(grad_block):
        left_gram = jnp.dot(grad_block, grad_block.T, preferred_element_type=jnp.float32)
        right_gram = jnp.dot(grad_block.T, grad_block, preferred_element_type=jnp.float32)
        return jnp.stack([left_gram, right_gram])
    grams = lax.map(gram_pair, grads).reshape(stat_count, block_width, block_width)
    new_stats = decay_rate * statistics + (1.0 - decay_rate) * grams
    slot_total = pending_stat.shape[0]
    slot_match = pending_stat[None, :] == jnp.arange(stat_count, dtype=jnp.int32)[:, None]
    found_slot = jnp.any(slot_match, axis=1)
    slot_of = lax.optimization_barrier(jnp.sum(jnp.where(slot_match, jnp.arange(slot_total, dtype=jnp.int32)[None, :], 0), axis=1)).astype(jnp.int32)
    returned = jnp.take(pending_roots, slot_of, axis=0)
    merged = jnp.where(found_slot[:, None, None], returned, held_roots)
    pairs = merged.reshape(stat_count // 2, 2, block_width, block_width)

    def precondition(item_pair):
        grad_block, root_pair = item_pair
        left_times = jnp.dot(root_pair[0], grad_block, preferred_element_type=jnp.float32).astype(jnp.bfloat16)
        product = jnp.dot(left_times, root_pair[1], preferred_element_type=jnp.float32)
        rms_scale = lax.rsqrt(jnp.mean(product * product) + 1e-06)
        return (product * rms_scale).astype(jnp.bfloat16)
    direction = lax.map(precondition, (grads, pairs)).reshape(-1, block_width)

    def refresh(slot_entry):
        statistic = lax.dynamic_index_in_dim(new_stats, jnp.maximum(slot_entry, 0), 0, keepdims=False)
        return lax.cond(slot_entry >= 0, lambda: inverse_root(statistic).astype(jnp.bfloat16), lambda: jnp.zeros((block_width, block_width), jnp.bfloat16))
    fresh = lax.map(refresh, refresh_stat)
    return (new_stats, merged, direction, fresh)
```

```python
import jax
import jax.numpy as jnp
from jax import lax
from jax.sharding import PartitionSpec as P

ITERS = 2


decay_rate = 0.9


def swapped(shard, axis, bit):
    return lax.ppermute(shard, axis, [(i, i ^ 1 << bit) for i in range(lax.axis_size(axis))])


def spread(parts):
    return lax.all_to_all(parts, "dev", split_axis=0, concat_axis=0, tiled=True)


def poly_times(first, second):
    result = [0.0] * (len(first) + len(second) - 1)
    for left_pos in range(len(first)):
        for right_pos in range(len(second)):
            result[left_pos + right_pos] += first[left_pos] * second[right_pos]
    return result


def root_polynomial(iteration_count):
    x_poly = [1.0]
    m_poly = [0.0, 1.0]
    for newton_turn in range(iteration_count):
        t_poly = [-value / 4.0 for value in m_poly]
        t_poly[0] += 5.0 / 4.0
        x_poly = poly_times(x_poly, t_poly)
        t_square = poly_times(t_poly, t_poly)
        m_poly = poly_times(poly_times(t_square, t_square), m_poly)
    return [float(value) for value in x_poly]


def matmul_exact(first, second):
    return jnp.dot(first, second, preferred_element_type=jnp.float32)


def inverse_root(statistic):
    size_b = statistic.shape[0]
    identity = jnp.eye(size_b, dtype=jnp.float32)
    norm_scale = 2.0 * jnp.trace(statistic) / size_b
    scaled = statistic / norm_scale
    coefficients = root_polynomial(ITERS)
    scaled_sq = matmul_exact(scaled, scaled)
    scaled_cube = matmul_exact(scaled_sq, scaled)
    lower_part = coefficients[0] * identity + coefficients[1] * scaled + coefficients[2] * scaled_sq
    upper_part = (
        coefficients[3] * identity
        + coefficients[4] * scaled
        + coefficients[5] * scaled_sq
        + coefficients[6] * scaled_cube
    )
    polynomial = lower_part + matmul_exact(scaled_cube, upper_part)
    return polynomial * norm_scale ** (-0.25)


def per_device(gradient, statistics, held_roots, pending_roots, pending_stat, refresh_stat):
    devices = lax.axis_size("dev")
    my_index = lax.axis_index("dev")
    parity = my_index % 2
    block_width = statistics.shape[1]
    piece_rows = block_width // devices
    slot_count = pending_roots.shape[0]
    half_rows = gradient.shape[0]
    slot_total = pending_stat.shape[0]

    pending_parts = spread(
        pending_roots.reshape(slot_count, devices, piece_rows, block_width).transpose(1, 0, 2, 3)
    ).reshape(slot_total, piece_rows, block_width)

    other_half = swapped(gradient, "dev", 0)
    top_half = jnp.where(parity == 0, gradient, other_half)
    bottom_half = jnp.where(parity == 0, other_half, gradient)
    full_grad = jnp.concatenate([top_half, bottom_half], axis=0)
    gram_term = lax.cond(
        parity == 0,
        lambda: lax.dot_general(
            full_grad, full_grad, (((1,), (1,)), ((), ())), preferred_element_type=jnp.float32
        ),
        lambda: lax.dot_general(
            full_grad, full_grad, (((0,), (0,)), ((), ())), preferred_element_type=jnp.float32
        ),
    )
    new_stat = decay_rate * statistics[0] + (1.0 - decay_rate) * gram_term
    my_root = lax.cond(
        jnp.any(refresh_stat == my_index),
        lambda: inverse_root(new_stat).astype(jnp.bfloat16),
        lambda: jnp.zeros(new_stat.shape, jnp.bfloat16),
    )
    root_parts = spread(my_root.reshape(devices, piece_rows, block_width))

    slot_match = pending_stat[None, :] == jnp.arange(devices, dtype=jnp.int32)[:, None]
    slot_of = jnp.sum(
        jnp.where(slot_match, jnp.arange(slot_total, dtype=jnp.int32)[None, :], 0), axis=1
    )
    returned = spread(jnp.take(pending_parts, slot_of, axis=0)).reshape(block_width, block_width)
    my_found = jnp.any(pending_stat == my_index)
    merged = jnp.where(my_found, returned, held_roots[0])

    routed = jnp.take(root_parts, jnp.maximum(refresh_stat, 0), axis=0)
    fresh = spread(routed.reshape(devices, slot_count, piece_rows, block_width))
    my_slots = lax.dynamic_slice_in_dim(refresh_stat, my_index * slot_count, slot_count, 0)
    fresh_roots = jnp.where(
        (my_slots >= 0)[:, None, None, None],
        fresh.transpose(1, 0, 2, 3),
        jnp.zeros((), jnp.bfloat16),
    ).reshape(slot_count, block_width, block_width)

    partner_root = swapped(merged, "dev", 0)
    left_root = jnp.where(parity == 0, merged, partner_root)
    right_root = jnp.where(parity == 0, partner_root, merged)
    left_rows = lax.dynamic_slice_in_dim(left_root, parity * half_rows, half_rows, 0)
    left_times = jnp.dot(left_rows, full_grad, preferred_element_type=jnp.float32).astype(
        jnp.bfloat16
    )
    product = jnp.dot(left_times, right_root, preferred_element_type=jnp.float32)
    own_square = jnp.sum(product * product)
    other_square = swapped(own_square, "dev", 0)
    rms_scale = lax.rsqrt((own_square + other_square) / (block_width * block_width) + 1e-06)
    direction = (product * rms_scale).astype(jnp.bfloat16)
    return (new_stat[None], merged[None], direction, fresh_roots)


def solution(mesh):
    in_specs = (
        P("dev", None),
        P("dev", None, None),
        P("dev", None, None),
        P("dev", None, None),
        P(),
        P(),
    )
    out_specs = (P("dev", None, None), P("dev", None, None), P("dev", None), P("dev", None, None))
    return jax.shard_map(
        per_device, mesh=mesh, in_specs=in_specs, out_specs=out_specs, check_vma=False
    )
```

```python
import functools

import jax
import jax.numpy as jnp
from jax import lax
from jax.experimental import pallas as pl
from jax.experimental.pallas import tpu as pltpu
from jax.sharding import PartitionSpec as P


ITERS = 2


decay_rate = 0.9


def swapped(shard, axis, bit):
    return lax.ppermute(shard, axis, [(i, i ^ 1 << bit) for i in range(lax.axis_size(axis))])


def spread(parts):
    return lax.all_to_all(parts, "dev", split_axis=0, concat_axis=0, tiled=True)


FIRST, OWN, SHARED, EXTRA = range(4)


def pick_kernel(width, kind_ref, row_ref, *refs):
    tables, out_ref, sem = refs[:-2], refs[-2], refs[-1]
    half = width // 2

    def issue(item, carry):
        kind, row = kind_ref[item], row_ref[item]

        def start(src, dst):
            pltpu.make_async_copy(src, dst, sem).start()

        @pl.when(kind == OWN)
        def _():
            start(tables[0].at[row, :, pl.ds(0, width)], out_ref.at[item])

        if len(tables) > 1:

            @pl.when(kind == FIRST)
            def _():
                start(tables[1].at[row], out_ref.at[item])

            @pl.when(kind == SHARED)
            def _():
                for core in range(2):
                    start(
                        tables[0].at[row // 2 * 2 + core, :, pl.ds(width, half)],
                        out_ref.at[item, :, pl.ds(core * half, half)],
                    )

        if len(tables) > 2:

            @pl.when(kind == EXTRA)
            def _():
                start(tables[2].at[row], out_ref.at[item])

        return carry

    lax.fori_loop(0, out_ref.shape[0], issue, 0, unroll=4)
    pltpu.make_async_copy(out_ref, out_ref, sem).wait()


def pick(kind, row, width, *tables):
    items, piece_rows = kind.shape[0], tables[0].shape[1]
    out_bytes = items * piece_rows * width * 2
    return pl.pallas_call(
        functools.partial(pick_kernel, width),
        out_shape=jax.ShapeDtypeStruct((items, piece_rows, width), tables[0].dtype),
        in_specs=[pl.BlockSpec(memory_space=pltpu.SMEM)] * 2
        + [pl.BlockSpec(memory_space=pl.ANY)] * len(tables),
        out_specs=pl.BlockSpec(memory_space=pltpu.VMEM),
        scratch_shapes=[pltpu.SemaphoreType.DMA],
        compiler_params=pltpu.CompilerParams(vmem_limit_bytes=16 * 1024 * 1024),
        cost_estimate=pl.CostEstimate(
            flops=4 * 1000 * 1000 * 1000, bytes_accessed=2 * out_bytes, transcendentals=0
        ),
        name="pick",
    )(kind, row, *tables)


def poly_times(first, second):
    result = [0.0] * (len(first) + len(second) - 1)
    for left_pos in range(len(first)):
        for right_pos in range(len(second)):
            result[left_pos + right_pos] += first[left_pos] * second[right_pos]
    return result


def root_polynomial(iteration_count):
    x_poly = [1.0]
    m_poly = [0.0, 1.0]
    for _ in range(iteration_count):
        t_poly = [-value / 4.0 for value in m_poly]
        t_poly[0] += 5.0 / 4.0
        x_poly = poly_times(x_poly, t_poly)
        t_square = poly_times(t_poly, t_poly)
        m_poly = poly_times(poly_times(t_square, t_square), m_poly)
    return [float(value) for value in x_poly]


def matmul_exact(first, second):
    return jnp.dot(first, second, preferred_element_type=jnp.float32)


def inverse_root(statistic):
    size_b = statistic.shape[0]
    identity = jnp.eye(size_b, dtype=jnp.float32)
    norm_scale = 2.0 * jnp.trace(statistic) / size_b
    scaled = statistic / norm_scale
    coefficients = root_polynomial(ITERS)
    scaled_sq = matmul_exact(scaled, scaled)
    scaled_cube = matmul_exact(scaled_sq, scaled)
    lower_part = coefficients[0] * identity + coefficients[1] * scaled + coefficients[2] * scaled_sq
    upper_part = (
        coefficients[3] * identity
        + coefficients[4] * scaled
        + coefficients[5] * scaled_sq
        + coefficients[6] * scaled_cube
    )
    polynomial = lower_part + matmul_exact(scaled_cube, upper_part)
    return polynomial * norm_scale ** (-0.25)


def per_device(gradient, statistics, held_roots, pending_roots, pending_stat, refresh_stat):
    devices = lax.axis_size("dev")
    my_index = lax.axis_index("dev")
    parity = my_index % 2
    block_width = statistics.shape[1]
    piece_rows = block_width // devices
    slot_count = pending_roots.shape[0]
    half_rows = gradient.shape[0]
    half_columns = block_width // 2
    slot_total = pending_stat.shape[0]
    device_ids = jnp.arange(devices, dtype=jnp.int32)

    has_first = pending_stat.reshape(devices, slot_count)[:, 0] >= 0
    has_second = has_first & (pending_stat.reshape(devices, slot_count)[:, 1] >= 0)
    refreshed = jnp.any(refresh_stat[None, :] == device_ids[:, None], axis=1)
    sharing = has_second & refreshed
    sharing_pairs = sharing.reshape(devices // 2, 2)
    unplaced = jnp.any(sharing_pairs[:, 0] & sharing_pairs[:, 1])

    my_first = lax.dynamic_slice_in_dim(pending_stat, my_index * slot_count, 1, 0)[0] >= 0
    first_root = lax.dynamic_index_in_dim(
        pending_roots, jnp.where(my_first, 0, 1), 0, keepdims=False
    )
    first_parts = spread(first_root.reshape(devices, piece_rows, block_width))

    other_half = swapped(gradient, "dev", 0)
    top_half = jnp.where(parity == 0, gradient, other_half)
    bottom_half = jnp.where(parity == 0, other_half, gradient)
    full_grad = jnp.concatenate([top_half, bottom_half], axis=0)
    gram_term = lax.cond(
        parity == 0,
        lambda: lax.dot_general(
            full_grad, full_grad, (((1,), (1,)), ((), ())), preferred_element_type=jnp.float32
        ),
        lambda: lax.dot_general(
            full_grad, full_grad, (((0,), (0,)), ((), ())), preferred_element_type=jnp.float32
        ),
    )
    new_stat = decay_rate * statistics[0] + (1.0 - decay_rate) * gram_term

    second_root = pending_roots[1]
    my_refreshed = jnp.any(refresh_stat == my_index)
    first_of_pair = lax.dynamic_slice_in_dim(sharing, my_index - parity, 1, 0)[0]
    from_other = jnp.where(first_of_pair, parity == 1, parity == 0)
    left_columns, right_columns = second_root[:, :half_columns], second_root[:, half_columns:]
    other_columns = swapped(jnp.where(parity == 0, right_columns, left_columns), "dev", 0)
    own_columns = jnp.where(parity == 0, left_columns, right_columns)
    shared_columns = jnp.where(from_other, other_columns, own_columns)
    own_matrix = lax.cond(
        my_refreshed, lambda: inverse_root(new_stat).astype(jnp.bfloat16), lambda: second_root
    )
    root_parts = spread(
        jnp.concatenate([own_matrix, shared_columns], axis=1).reshape(
            devices, piece_rows, block_width + half_columns
        ),
    )

    slot_match = pending_stat[None, :] == device_ids[:, None]
    slot_of = jnp.sum(
        jnp.where(slot_match, jnp.arange(slot_total, dtype=jnp.int32)[None, :], 0), axis=1
    )
    source = slot_of // slot_count
    is_second = jnp.any(
        slot_match & (jnp.arange(slot_total) % slot_count == 1) & jnp.repeat(has_first, slot_count),
        axis=1,
    )
    is_shared = jnp.any(slot_match & jnp.repeat(refreshed, slot_count), axis=1)
    is_extra = jnp.any(
        slot_match
        & (jnp.arange(slot_total) // slot_count % 2 == 1)
        & jnp.repeat(jnp.repeat(sharing_pairs[:, 0], 2), slot_count),
        axis=1,
    )
    kind = jnp.where(is_second, jnp.where(is_shared, SHARED, OWN), FIRST).astype(jnp.int32)
    kind_extra = jnp.where(is_second & is_shared & is_extra, EXTRA, kind).astype(jnp.int32)
    chosen = lax.cond(
        unplaced,
        lambda: pick(
            kind_extra,
            source,
            block_width,
            root_parts,
            first_parts,
            spread(second_root.reshape(devices, piece_rows, block_width)),
        ),
        lambda: pick(kind, source, block_width, root_parts, first_parts),
    )
    returned = spread(chosen).reshape(block_width, block_width)
    my_found = jnp.any(pending_stat == my_index)
    merged = jnp.where(my_found, returned, held_roots[0])

    routed = pick(
        jnp.full((slot_total,), OWN, jnp.int32),
        jnp.maximum(refresh_stat, 0),
        block_width,
        root_parts,
    )
    fresh = spread(routed.reshape(devices, slot_count, piece_rows, block_width))

    partner_root = swapped(merged, "dev", 0)
    left_root = jnp.where(parity == 0, merged, partner_root)
    right_root = jnp.where(parity == 0, partner_root, merged)
    left_rows = lax.dynamic_slice_in_dim(left_root, parity * half_rows, half_rows, 0)
    left_times = jnp.dot(left_rows, full_grad, preferred_element_type=jnp.float32).astype(
        jnp.bfloat16
    )
    product = jnp.dot(left_times, right_root, preferred_element_type=jnp.float32)
    own_square = jnp.sum(product * product)
    other_square = swapped(own_square, "dev", 0)
    rms_scale = lax.rsqrt((own_square + other_square) / (block_width * block_width) + 1e-06)
    direction = (product * rms_scale).astype(jnp.bfloat16)

    fresh, direction = lax.optimization_barrier((fresh, direction))
    my_slots = lax.dynamic_slice_in_dim(refresh_stat, my_index * slot_count, slot_count, 0)
    fresh_roots = jnp.where(
        (my_slots >= 0)[:, None, None, None],
        fresh.transpose(1, 0, 2, 3),
        jnp.zeros((), jnp.bfloat16),
    ).reshape(slot_count, block_width, block_width)
    return (new_stat[None], merged[None], direction, fresh_roots)


def solution(mesh):
    in_specs = (
        P("dev", None),
        P("dev", None, None),
        P("dev", None, None),
        P("dev", None, None),
        P(),
        P(),
    )
    out_specs = (P("dev", None, None), P("dev", None, None), P("dev", None), P("dev", None, None))
    return jax.shard_map(
        per_device, mesh=mesh, in_specs=in_specs, out_specs=out_specs, check_vma=False
    )
```

```python
import functools

import jax
import jax.numpy as jnp
from jax import lax
from jax.experimental import pallas as pl
from jax.experimental.pallas import tpu as pltpu
from jax.sharding import PartitionSpec as P


ITERS = 2


decay_rate = 0.9


def swapped(shard, axis, bit):
    return lax.ppermute(shard, axis, [(i, i ^ 1 << bit) for i in range(lax.axis_size(axis))])


def spread(parts):
    return lax.all_to_all(parts, "dev", split_axis=0, concat_axis=0, tiled=True)


FIRST, OWN, SHARED, EXTRA = range(4)


def pick_kernel(width, kind_ref, row_ref, *refs):
    tables, out_ref, sem = refs[:-2], refs[-2], refs[-1]
    half = width // 2

    def start(src, dst):
        pltpu.make_async_copy(src, dst, sem).start()

    def issue(item, carry):
        row = row_ref[item]
        if len(tables) == 1:
            start(tables[0].at[row, :, pl.ds(0, width)], out_ref.at[item])
            return carry
        kind = kind_ref[item]

        @pl.when(kind == FIRST)
        def _():
            start(tables[1].at[row], out_ref.at[item])

        @pl.when(kind != FIRST)
        def _():
            @pl.when(kind == OWN)
            def _():
                start(tables[0].at[row, :, pl.ds(0, width)], out_ref.at[item])

            @pl.when(kind == SHARED)
            def _():
                for core in range(2):
                    start(
                        tables[0].at[row // 2 * 2 + core, :, pl.ds(width, half)],
                        out_ref.at[item, :, pl.ds(core * half, half)],
                    )

            if len(tables) > 2:

                @pl.when(kind == EXTRA)
                def _():
                    start(tables[2].at[row], out_ref.at[item])

        return carry

    lax.fori_loop(0, out_ref.shape[0], issue, 0, unroll=8)
    pltpu.make_async_copy(out_ref, out_ref, sem).wait()


def pick(kind, row, width, *tables):
    items, piece_rows = row.shape[0], tables[0].shape[1]
    out_bytes = items * piece_rows * width * 2
    return pl.pallas_call(
        functools.partial(pick_kernel, width),
        out_shape=jax.ShapeDtypeStruct((items, piece_rows, width), tables[0].dtype),
        in_specs=[pl.BlockSpec(memory_space=pltpu.SMEM)] * 2
        + [pl.BlockSpec(memory_space=pl.ANY)] * len(tables),
        out_specs=pl.BlockSpec(memory_space=pltpu.VMEM),
        scratch_shapes=[pltpu.SemaphoreType.DMA],
        compiler_params=pltpu.CompilerParams(vmem_limit_bytes=16 * 1024 * 1024),
        cost_estimate=pl.CostEstimate(
            flops=4 * 1000 * 1000 * 1000, bytes_accessed=2 * out_bytes, transcendentals=0
        ),
        name="pick",
    )(kind, row, *tables)


def first_kernel(index_ref, stat_ref, pending_ref, out_ref, sem):
    slot = jnp.where(stat_ref[index_ref[0] * 2] >= 0, 0, 1)
    copy = pltpu.make_async_copy(pending_ref.at[slot], out_ref, sem)
    copy.start()
    copy.wait()


def first_used(my_index, pending_stat, pending_roots):
    return pl.pallas_call(
        first_kernel,
        out_shape=jax.ShapeDtypeStruct(pending_roots.shape[1:], pending_roots.dtype),
        in_specs=[pl.BlockSpec(memory_space=pltpu.SMEM)] * 2
        + [pl.BlockSpec(memory_space=pl.ANY)],
        out_specs=pl.BlockSpec(memory_space=pltpu.VMEM),
        scratch_shapes=[pltpu.SemaphoreType.DMA],
        compiler_params=pltpu.CompilerParams(vmem_limit_bytes=8 * 1024 * 1024),
        name="first_used",
    )(my_index.reshape(1), pending_stat, pending_roots)


def poly_times(first, second):
    result = [0.0] * (len(first) + len(second) - 1)
    for left_pos in range(len(first)):
        for right_pos in range(len(second)):
            result[left_pos + right_pos] += first[left_pos] * second[right_pos]
    return result


def root_polynomial(iteration_count):
    x_poly = [1.0]
    m_poly = [0.0, 1.0]
    for _ in range(iteration_count):
        t_poly = [-value / 4.0 for value in m_poly]
        t_poly[0] += 5.0 / 4.0
        x_poly = poly_times(x_poly, t_poly)
        t_square = poly_times(t_poly, t_poly)
        m_poly = poly_times(poly_times(t_square, t_square), m_poly)
    return [float(value) for value in x_poly]


TILE = 256


def root_kernel(
    flag_ref,
    gram_ref,
    stat_ref,
    pending_ref,
    other_ref,
    new_ref,
    own_ref,
    scaled_ref,
    scaled16_ref,
    square_ref,
    square16_ref,
    cube16_ref,
    upper_ref,
    diagonal_ref,
    sems,
):
    width = stat_ref.shape[0]
    half = width // 2
    refreshed, from_other, parity = flag_ref[0], flag_ref[1], flag_ref[2]
    poly = root_polynomial(ITERS)
    shared = own_ref.at[:, pl.ds(width, half)]

    @pl.when(from_other > 0)
    def _():
        pltpu.make_async_copy(other_ref, shared, sems.at[0]).start()

    @pl.when(from_other == 0)
    def _():
        columns = pl.ds(pl.multiple_of(parity * half, half), half)
        pltpu.make_async_copy(pending_ref.at[1, :, columns], shared, sems.at[0]).start()

    second = pltpu.make_async_copy(pending_ref.at[1], own_ref.at[:, pl.ds(0, width)], sems.at[1])

    @pl.when(refreshed == 0)
    def _():
        second.start()

    diagonal_ref[...] = jnp.zeros_like(diagonal_ref)

    @pl.loop(0, width // 128)
    def _(step):
        rows = pl.ds(pl.multiple_of(step * 128, 128), 128)
        new_ref[rows, :] = decay_rate * stat_ref[rows, :] + (1.0 - decay_rate) * gram_ref[rows, :]
        on_diagonal = lax.broadcasted_iota(jnp.int32, (128, 128), 0) == lax.broadcasted_iota(
            jnp.int32, (128, 128), 1
        )
        diagonal_ref[...] += jnp.where(on_diagonal, new_ref[rows, rows], 0.0)

    @pl.when(refreshed > 0)
    def _():
        trace = jnp.sum(jnp.sum(diagonal_ref[...], axis=1, keepdims=True), axis=0, keepdims=True)
        norm_scale = 2.0 * trace / width
        factor = lax.rsqrt(jnp.sqrt(norm_scale))

        @pl.loop(0, width // 128)
        def _(step):
            rows = pl.ds(pl.multiple_of(step * 128, 128), 128)
            scaled = new_ref[rows, :] / norm_scale
            scaled_ref[rows, :] = scaled
            scaled16_ref[rows, :] = scaled.astype(jnp.bfloat16)

        def columns_of(step):
            return pl.ds(pl.multiple_of(step * TILE, TILE), TILE)

        def identity(step):
            return (
                lax.broadcasted_iota(jnp.int32, (width, TILE), 0)
                == lax.broadcasted_iota(jnp.int32, (width, TILE), 1) + step * TILE
            )

        def dot(first, second):
            return jnp.dot(first, second, preferred_element_type=jnp.float32)

        @pl.loop(0, width // TILE)
        def _(step):
            columns = columns_of(step)
            square = dot(scaled16_ref[...], scaled16_ref[:, columns])
            square_ref[:, columns] = square
            square16_ref[:, columns] = square.astype(jnp.bfloat16)

        @pl.loop(0, width // TILE)
        def _(step):
            columns = columns_of(step)
            cube = dot(square16_ref[...], scaled16_ref[:, columns])
            cube16_ref[:, columns] = cube.astype(jnp.bfloat16)
            upper = (
                jnp.where(identity(step), poly[3], 0.0)
                + poly[4] * scaled_ref[:, columns]
                + poly[5] * square_ref[:, columns]
                + poly[6] * cube
            )
            upper_ref[:, columns] = upper.astype(jnp.bfloat16)

        @pl.loop(0, width // TILE)
        def _(step):
            columns = columns_of(step)
            total = dot(cube16_ref[...], upper_ref[:, columns])
            total += (
                jnp.where(identity(step), poly[0], 0.0)
                + poly[1] * scaled_ref[:, columns]
                + poly[2] * square_ref[:, columns]
            )
            own_ref[:, columns] = (total * factor).astype(jnp.bfloat16)

    @pl.when(refreshed == 0)
    def _():
        second.wait()

    pltpu.make_async_copy(other_ref, shared, sems.at[0]).wait()


def updated_and_root(flags, gram, statistic, pending_roots, other_columns):
    width = statistic.shape[0]
    vmem = pl.BlockSpec(memory_space=pltpu.VMEM)
    anywhere = pl.BlockSpec(memory_space=pl.ANY)
    return pl.pallas_call(
        root_kernel,
        out_shape=(
            jax.ShapeDtypeStruct((width, width), jnp.float32),
            jax.ShapeDtypeStruct((width, width + width // 2), jnp.bfloat16),
        ),
        in_specs=[pl.BlockSpec(memory_space=pltpu.SMEM), vmem, vmem, anywhere, anywhere],
        out_specs=(vmem, vmem),
        scratch_shapes=[
            pltpu.VMEM((width, width), jnp.float32),
            pltpu.VMEM((width, width), jnp.bfloat16),
            pltpu.VMEM((width, width), jnp.float32),
            pltpu.VMEM((width, width), jnp.bfloat16),
            pltpu.VMEM((width, width), jnp.bfloat16),
            pltpu.VMEM((width, width), jnp.bfloat16),
            pltpu.VMEM((128, 128), jnp.float32),
            pltpu.SemaphoreType.DMA((2,)),
        ],
        compiler_params=pltpu.CompilerParams(vmem_limit_bytes=44 * 1024 * 1024),
        cost_estimate=pl.CostEstimate(
            flops=6 * width**3, bytes_accessed=15 * width * width, transcendentals=0
        ),
        name="root",
    )(flags, gram, statistic, pending_roots, other_columns)


def per_device(gradient, statistics, held_roots, pending_roots, pending_stat, refresh_stat):
    devices = lax.axis_size("dev")
    my_index = lax.axis_index("dev")
    parity = my_index % 2
    block_width = statistics.shape[1]
    piece_rows = block_width // devices
    slot_count = pending_roots.shape[0]
    half_rows = gradient.shape[0]
    half_columns = block_width // 2
    slot_total = pending_stat.shape[0]
    device_ids = jnp.arange(devices, dtype=jnp.int32)

    has_first = pending_stat.reshape(devices, slot_count)[:, 0] >= 0
    has_second = has_first & (pending_stat.reshape(devices, slot_count)[:, 1] >= 0)
    refreshed = jnp.any(refresh_stat[None, :] == device_ids[:, None], axis=1)
    sharing = has_second & refreshed
    sharing_pairs = sharing.reshape(devices // 2, 2)
    unplaced = jnp.any(sharing_pairs[:, 0] & sharing_pairs[:, 1])

    first_root = first_used(my_index, pending_stat, pending_roots)
    first_parts = spread(first_root.reshape(devices, piece_rows, block_width))

    other_half = swapped(gradient, "dev", 0)
    top_half = jnp.where(parity == 0, gradient, other_half)
    bottom_half = jnp.where(parity == 0, other_half, gradient)
    full_grad = jnp.concatenate([top_half, bottom_half], axis=0)
    gram_term = lax.cond(
        parity == 0,
        lambda: lax.dot_general(
            full_grad, full_grad, (((1,), (1,)), ((), ())), preferred_element_type=jnp.float32
        ),
        lambda: lax.dot_general(
            full_grad, full_grad, (((0,), (0,)), ((), ())), preferred_element_type=jnp.float32
        ),
    )
    second_root = pending_roots[1]
    my_refreshed = jnp.any(refresh_stat == my_index)
    first_of_pair = lax.dynamic_slice_in_dim(sharing, my_index - parity, 1, 0)[0]
    from_other = jnp.where(first_of_pair, parity == 1, parity == 0)
    other_columns = swapped(
        lax.dynamic_slice(
            pending_roots, (1, 0, (1 - parity) * half_columns), (1, block_width, half_columns)
        )[0],
        "dev",
        0,
    )
    flags = jnp.stack([my_refreshed, from_other, parity]).astype(jnp.int32)
    new_stat, own_matrix = updated_and_root(
        flags, gram_term, statistics[0], pending_roots, other_columns
    )
    root_parts = spread(own_matrix.reshape(devices, piece_rows, block_width + half_columns))

    slot_match = pending_stat[None, :] == device_ids[:, None]
    slot_of = jnp.sum(
        jnp.where(slot_match, jnp.arange(slot_total, dtype=jnp.int32)[None, :], 0), axis=1
    )
    source = slot_of // slot_count
    is_second = jnp.any(
        slot_match & (jnp.arange(slot_total) % slot_count == 1) & jnp.repeat(has_first, slot_count),
        axis=1,
    )
    is_shared = jnp.any(slot_match & jnp.repeat(refreshed, slot_count), axis=1)
    is_extra = jnp.any(
        slot_match
        & (jnp.arange(slot_total) // slot_count % 2 == 1)
        & jnp.repeat(jnp.repeat(sharing_pairs[:, 0], 2), slot_count),
        axis=1,
    )
    kind = jnp.where(is_second, jnp.where(is_shared, SHARED, OWN), FIRST).astype(jnp.int32)
    kind_extra = jnp.where(is_second & is_shared & is_extra, EXTRA, kind).astype(jnp.int32)
    chosen = lax.cond(
        unplaced,
        lambda: pick(
            kind_extra,
            source,
            block_width,
            root_parts,
            first_parts,
            spread(second_root.reshape(devices, piece_rows, block_width)),
        ),
        lambda: pick(kind, source, block_width, root_parts, first_parts),
    )
    returned = spread(chosen).reshape(block_width, block_width)
    my_found = jnp.any(pending_stat == my_index)
    merged = jnp.where(my_found, returned, held_roots[0])

    routed = pick(
        jnp.full((slot_total,), OWN, jnp.int32),
        jnp.maximum(refresh_stat, 0),
        block_width,
        root_parts,
    )
    fresh = spread(routed.reshape(devices, slot_count, piece_rows, block_width))

    partner_root = swapped(merged, "dev", 0)
    left_root = jnp.where(parity == 0, merged, partner_root)
    right_root = jnp.where(parity == 0, partner_root, merged)
    left_rows = lax.dynamic_slice_in_dim(left_root, parity * half_rows, half_rows, 0)
    left_times = jnp.dot(left_rows, full_grad, preferred_element_type=jnp.float32).astype(
        jnp.bfloat16
    )
    product = jnp.dot(left_times, right_root, preferred_element_type=jnp.float32)
    own_square = jnp.sum(product * product)
    other_square = swapped(own_square, "dev", 0)
    rms_scale = lax.rsqrt((own_square + other_square) / (block_width * block_width) + 1e-06)
    direction = (product * rms_scale).astype(jnp.bfloat16)

    fresh, direction = lax.optimization_barrier((fresh, direction))
    my_slots = lax.dynamic_slice_in_dim(refresh_stat, my_index * slot_count, slot_count, 0)
    fresh_roots = jnp.where(
        (my_slots >= 0)[:, None, None, None],
        fresh.transpose(1, 0, 2, 3),
        jnp.zeros((), jnp.bfloat16),
    ).reshape(slot_count, block_width, block_width)
    return (new_stat[None], merged[None], direction, fresh_roots)


def solution(mesh):
    in_specs = (
        P("dev", None),
        P("dev", None, None),
        P("dev", None, None),
        P("dev", None, None),
        P(),
        P(),
    )
    out_specs = (P("dev", None, None), P("dev", None, None), P("dev", None), P("dev", None, None))
    return jax.shard_map(
        per_device, mesh=mesh, in_specs=in_specs, out_specs=out_specs, check_vma=False
    )
```

```python
import functools

import jax
import jax.numpy as jnp
from jax import lax
from jax.experimental import pallas as pl
from jax.experimental.pallas import tpu as pltpu
from jax.sharding import PartitionSpec as P


ITERS = 2


decay_rate = 0.9


def swapped(shard, axis, bit):
    return lax.ppermute(shard, axis, [(i, i ^ 1 << bit) for i in range(lax.axis_size(axis))])


def spread(parts):
    return lax.all_to_all(parts, "dev", split_axis=0, concat_axis=0, tiled=True)


FIRST, OWN, SHARED, EXTRA = range(4)


def pick_kernel(width, kind_ref, row_ref, *refs):
    tables, out_ref, sem = refs[:-2], refs[-2], refs[-1]
    half = width // 2

    def start(src, dst):
        pltpu.make_async_copy(src, dst, sem).start()

    def issue(item, carry):
        row = row_ref[item]
        if len(tables) == 1:
            start(tables[0].at[row, :, pl.ds(0, width)], out_ref.at[item])
            return carry
        kind = kind_ref[item]

        @pl.when(kind == FIRST)
        def _():
            start(tables[1].at[row], out_ref.at[item])

        @pl.when(kind != FIRST)
        def _():
            @pl.when(kind == OWN)
            def _():
                start(tables[0].at[row, :, pl.ds(0, width)], out_ref.at[item])

            @pl.when(kind == SHARED)
            def _():
                for core in range(2):
                    start(
                        tables[0].at[row // 2 * 2 + core, :, pl.ds(width, half)],
                        out_ref.at[item, :, pl.ds(core * half, half)],
                    )

            if len(tables) > 2:

                @pl.when(kind == EXTRA)
                def _():
                    start(tables[2].at[row], out_ref.at[item])

        return carry

    lax.fori_loop(0, out_ref.shape[0], issue, 0, unroll=8)
    pltpu.make_async_copy(out_ref, out_ref, sem).wait()


def pick(kind, row, width, *tables):
    items, piece_rows = row.shape[0], tables[0].shape[1]
    out_bytes = items * piece_rows * width * 2
    return pl.pallas_call(
        functools.partial(pick_kernel, width),
        out_shape=jax.ShapeDtypeStruct((items, piece_rows, width), tables[0].dtype),
        in_specs=[pl.BlockSpec(memory_space=pltpu.SMEM)] * 2
        + [pl.BlockSpec(memory_space=pl.ANY)] * len(tables),
        out_specs=pl.BlockSpec(memory_space=pltpu.VMEM),
        scratch_shapes=[pltpu.SemaphoreType.DMA],
        compiler_params=pltpu.CompilerParams(vmem_limit_bytes=16 * 1024 * 1024),
        cost_estimate=pl.CostEstimate(
            flops=4 * 1000 * 1000 * 1000, bytes_accessed=2 * out_bytes, transcendentals=0
        ),
        name="pick",
    )(kind, row, *tables)


CHUNKS = 4


def first_kernel(index_ref, stat_ref, pending_ref, first_ref, columns_ref, held, cut, sems):
    rows, width = first_ref.shape
    half, step = width // 2, rows // CHUNKS
    slot = jnp.where(stat_ref[index_ref[0] * 2] >= 0, 0, 1)
    other_half = pl.ds(pl.multiple_of((1 - index_ref[0] % 2) * half, half), half)
    moves = []
    for chunk in range(CHUNKS):
        part = pl.ds(chunk * step, step)
        moves.append((pending_ref.at[slot, part, :], held.at[part, :], first_ref.at[part, :]))
    moves.append((pending_ref.at[1, :, other_half], cut, columns_ref))
    loads = [
        pltpu.make_async_copy(src, mid, sems.at[0, pos]) for pos, (src, mid, dst) in enumerate(moves)
    ]
    stores = [
        pltpu.make_async_copy(mid, dst, sems.at[1, pos]) for pos, (src, mid, dst) in enumerate(moves)
    ]
    for load in loads:
        load.start()
    for load, store in zip(loads, stores):
        load.wait()
        store.start()
    for store in stores:
        store.wait()


def first_used(my_index, pending_stat, pending_roots):
    rows, width = pending_roots.shape[1:]
    kind = pending_roots.dtype
    anywhere = pl.BlockSpec(memory_space=pl.ANY)
    return pl.pallas_call(
        first_kernel,
        out_shape=(
            jax.ShapeDtypeStruct((rows, width), kind),
            jax.ShapeDtypeStruct((rows, width // 2), kind),
        ),
        in_specs=[pl.BlockSpec(memory_space=pltpu.SMEM)] * 2 + [anywhere],
        out_specs=(anywhere, anywhere),
        scratch_shapes=[
            pltpu.VMEM((rows, width), kind),
            pltpu.VMEM((rows, width // 2), kind),
            pltpu.SemaphoreType.DMA((2, CHUNKS + 1)),
        ],
        compiler_params=pltpu.CompilerParams(vmem_limit_bytes=8 * 1024 * 1024),
        name="first_used",
    )(my_index, pending_stat, pending_roots)


def poly_times(first, second):
    result = [0.0] * (len(first) + len(second) - 1)
    for left_pos in range(len(first)):
        for right_pos in range(len(second)):
            result[left_pos + right_pos] += first[left_pos] * second[right_pos]
    return result


def root_polynomial(iteration_count):
    x_poly = [1.0]
    m_poly = [0.0, 1.0]
    for _ in range(iteration_count):
        t_poly = [-value / 4.0 for value in m_poly]
        t_poly[0] += 5.0 / 4.0
        x_poly = poly_times(x_poly, t_poly)
        t_square = poly_times(t_poly, t_poly)
        m_poly = poly_times(poly_times(t_square, t_square), m_poly)
    return [float(value) for value in x_poly]


TILE = 256


def root_kernel(
    index_ref,
    pending_stat_ref,
    refresh_stat_ref,
    own_grad_ref,
    other_grad_ref,
    stat_ref,
    pending_ref,
    other_ref,
    new_ref,
    own_ref,
    grad_ref,
    grad,
    factor16,
    stat,
    scaled,
    scaled16,
    square,
    square16,
    cube16,
    upper16,
    root16,
    shared,
    sems,
):
    width = stat_ref.shape[0]
    half = width // 2
    tiles = width // TILE
    me = index_ref[0]
    parity = me % 2
    poly = root_polynomial(ITERS)

    def columns_of(step):
        return pl.ds(pl.multiple_of(step * TILE, TILE), TILE)

    def half_of(side):
        return pl.ds(pl.multiple_of(side * half, half), half)

    own_half = pltpu.make_async_copy(own_grad_ref, grad.at[half_of(parity), :], sems.at[0])
    other_half = pltpu.make_async_copy(other_grad_ref, grad.at[half_of(1 - parity), :], sems.at[1])
    statistic = pltpu.make_async_copy(stat_ref, stat, sems.at[2])
    grad_out = pltpu.make_async_copy(grad, grad_ref, sems.at[3])
    new_out = pltpu.make_async_copy(stat, new_ref, sems.at[4])
    second = pltpu.make_async_copy(pending_ref.at[1], root16, sems.at[5])
    shared_in = pltpu.make_async_copy(other_ref, shared, sems.at[6])
    shared_out = pltpu.make_async_copy(shared, own_ref.at[:, pl.ds(width, half)], sems.at[7])

    def root_out(step):
        return pltpu.make_async_copy(
            root16.at[:, columns_of(step)], own_ref.at[:, columns_of(step)], sems.at[8]
        )

    own_half.start()
    other_half.start()
    statistic.start()

    def look(item, found):
        entry = refresh_stat_ref[item]
        return found[0] | (entry == me), found[1] | (entry == me - parity)

    refreshed, core_refreshed = lax.fori_loop(
        0, refresh_stat_ref.shape[0], look, (jnp.bool_(False), jnp.bool_(False)), unroll=16
    )
    core = (me - parity) * 2
    core_shares = (
        core_refreshed & (pending_stat_ref[core] >= 0) & (pending_stat_ref[core + 1] >= 0)
    )
    from_other = core_shares == (parity == 1)

    @pl.when(from_other)
    def _():
        shared_in.start()

    @pl.when(jnp.logical_not(from_other))
    def _():
        pltpu.make_async_copy(
            pending_ref.at[1, :, half_of(parity)], shared, sems.at[6]
        ).start()

    @pl.when(jnp.logical_not(refreshed))
    def _():
        second.start()

    own_half.wait()
    other_half.wait()
    grad_out.start()

    @pl.when(parity == 0)
    def _():
        factor16[...] = grad[...]

    @pl.when(parity == 1)
    def _():
        @pl.loop(0, tiles)
        def _(step):
            columns = columns_of(step)
            factor16[columns, :] = jnp.transpose(grad[:, columns])

    statistic.wait()

    def update(step, trace):
        columns = columns_of(step)
        gram = lax.dot_general(
            factor16[...],
            factor16[columns, :],
            (((1,), (1,)), ((), ())),
            preferred_element_type=jnp.float32,
        )
        stat[:, columns] = decay_rate * stat[:, columns] + (1.0 - decay_rate) * gram
        block = stat[columns, columns]
        on_diagonal = lax.broadcasted_iota(jnp.int32, (TILE, TILE), 0) == lax.broadcasted_iota(
            jnp.int32, (TILE, TILE), 1
        )
        return trace + jnp.sum(jnp.where(on_diagonal, block, 0.0), axis=0, keepdims=True)

    diagonal = lax.fori_loop(0, tiles, update, jnp.zeros((1, TILE), jnp.float32))
    shared_in.wait()
    shared_out.start()

    @pl.when(jnp.logical_not(refreshed))
    def _():
        second.wait()
        new_out.start()
        for step in range(tiles):
            root_out(step).start()

    @pl.when(refreshed)
    def _():
        norm_scale = 2.0 * jnp.sum(diagonal, axis=1, keepdims=True) / width
        factor = lax.rsqrt(jnp.sqrt(norm_scale))

        @pl.loop(0, width // 128)
        def _(step):
            rows = pl.ds(pl.multiple_of(step * 128, 128), 128)
            part = stat[rows, :] / norm_scale
            scaled[rows, :] = part
            scaled16[rows, :] = part.astype(jnp.bfloat16)

        new_out.start()

        def identity(step):
            return (
                lax.broadcasted_iota(jnp.int32, (width, TILE), 0)
                == lax.broadcasted_iota(jnp.int32, (width, TILE), 1) + step * TILE
            )

        def dot(first, second):
            return jnp.dot(first, second, preferred_element_type=jnp.float32)

        @pl.loop(0, tiles)
        def _(step):
            columns = columns_of(step)
            tile = dot(scaled16[...], scaled16[:, columns])
            square[:, columns] = tile
            square16[:, columns] = tile.astype(jnp.bfloat16)

        @pl.loop(0, tiles)
        def _(step):
            columns = columns_of(step)
            cube = dot(square16[...], scaled16[:, columns])
            cube16[:, columns] = cube.astype(jnp.bfloat16)
            upper = (
                jnp.where(identity(step), poly[3], 0.0)
                + poly[4] * scaled[:, columns]
                + poly[5] * square[:, columns]
                + poly[6] * cube
            )
            upper16[:, columns] = upper.astype(jnp.bfloat16)

        @pl.loop(0, tiles)
        def _(step):
            columns = columns_of(step)
            total = dot(cube16[...], upper16[:, columns])
            total += (
                jnp.where(identity(step), poly[0], 0.0)
                + poly[1] * scaled[:, columns]
                + poly[2] * square[:, columns]
            )
            root16[:, columns] = (total * factor).astype(jnp.bfloat16)

            @pl.when(step > 0)
            def _():
                root_out(step - 1).start()

    grad_out.wait()
    new_out.wait()

    @pl.when(refreshed)
    def _():
        root_out(tiles - 1).start()

    shared_out.wait()
    pltpu.make_async_copy(root16, own_ref.at[:, pl.ds(0, width)], sems.at[8]).wait()


def updated_and_root(
    my_index, pending_stat, refresh_stat, own_grad, other_grad, statistic, pending_roots, columns
):
    width = statistic.shape[0]
    anywhere = pl.BlockSpec(memory_space=pl.ANY)
    plain = pltpu.VMEM((width, width), jnp.float32)
    short = pltpu.VMEM((width, width), jnp.bfloat16)
    return pl.pallas_call(
        root_kernel,
        out_shape=(
            jax.ShapeDtypeStruct((width, width), jnp.float32),
            jax.ShapeDtypeStruct((width, width + width // 2), jnp.bfloat16),
            jax.ShapeDtypeStruct((width, width), jnp.bfloat16),
        ),
        in_specs=[pl.BlockSpec(memory_space=pltpu.SMEM)] * 3 + [anywhere] * 5,
        out_specs=(anywhere,) * 3,
        scratch_shapes=[
            short,
            short,
            plain,
            plain,
            short,
            plain,
            short,
            short,
            short,
            short,
            pltpu.VMEM((width, width // 2), jnp.bfloat16),
            pltpu.SemaphoreType.DMA((9,)),
        ],
        compiler_params=pltpu.CompilerParams(vmem_limit_bytes=44 * 1024 * 1024),
        cost_estimate=pl.CostEstimate(
            flops=8 * width**3, bytes_accessed=17 * width * width, transcendentals=0
        ),
        name="root",
    )(
        my_index,
        pending_stat,
        refresh_stat,
        own_grad,
        other_grad,
        statistic,
        pending_roots,
        columns,
    )


def per_device(gradient, statistics, held_roots, pending_roots, pending_stat, refresh_stat):
    devices = lax.axis_size("dev")
    my_index = lax.axis_index("dev")
    parity = my_index % 2
    block_width = statistics.shape[1]
    piece_rows = block_width // devices
    slot_count = pending_roots.shape[0]
    half_rows = gradient.shape[0]
    half_columns = block_width // 2
    slot_total = pending_stat.shape[0]
    device_ids = jnp.arange(devices, dtype=jnp.int32)

    has_first = pending_stat.reshape(devices, slot_count)[:, 0] >= 0
    has_second = has_first & (pending_stat.reshape(devices, slot_count)[:, 1] >= 0)
    refreshed = jnp.any(refresh_stat[None, :] == device_ids[:, None], axis=1)
    sharing = has_second & refreshed
    sharing_pairs = sharing.reshape(devices // 2, 2)
    unplaced = jnp.any(sharing_pairs[:, 0] & sharing_pairs[:, 1])

    index_table = my_index.reshape(1)
    first_root, cut_columns = first_used(index_table, pending_stat, pending_roots)
    first_parts = spread(first_root.reshape(devices, piece_rows, block_width))

    new_stat, own_matrix, full_grad = updated_and_root(
        index_table,
        pending_stat,
        refresh_stat,
        gradient,
        swapped(gradient, "dev", 0),
        statistics[0],
        pending_roots,
        swapped(cut_columns, "dev", 0),
    )
    second_root = pending_roots[1]
    root_parts = spread(own_matrix.reshape(devices, piece_rows, block_width + half_columns))

    slot_match = pending_stat[None, :] == device_ids[:, None]
    slot_of = jnp.sum(
        jnp.where(slot_match, jnp.arange(slot_total, dtype=jnp.int32)[None, :], 0), axis=1
    )
    source = slot_of // slot_count
    is_second = jnp.any(
        slot_match & (jnp.arange(slot_total) % slot_count == 1) & jnp.repeat(has_first, slot_count),
        axis=1,
    )
    is_shared = jnp.any(slot_match & jnp.repeat(refreshed, slot_count), axis=1)
    is_extra = jnp.any(
        slot_match
        & (jnp.arange(slot_total) // slot_count % 2 == 1)
        & jnp.repeat(jnp.repeat(sharing_pairs[:, 0], 2), slot_count),
        axis=1,
    )
    kind = jnp.where(is_second, jnp.where(is_shared, SHARED, OWN), FIRST).astype(jnp.int32)
    kind_extra = jnp.where(is_second & is_shared & is_extra, EXTRA, kind).astype(jnp.int32)
    chosen = lax.cond(
        unplaced,
        lambda: pick(
            kind_extra,
            source,
            block_width,
            root_parts,
            first_parts,
            spread(second_root.reshape(devices, piece_rows, block_width)),
        ),
        lambda: pick(kind, source, block_width, root_parts, first_parts),
    )
    returned = spread(chosen).reshape(block_width, block_width)
    my_found = jnp.any(pending_stat == my_index)
    merged = jnp.where(my_found, returned, held_roots[0])

    routed = pick(
        jnp.full((slot_total,), OWN, jnp.int32),
        jnp.maximum(refresh_stat, 0),
        block_width,
        root_parts,
    )
    fresh = spread(routed.reshape(devices, slot_count, piece_rows, block_width))

    partner_root = swapped(merged, "dev", 0)
    left_root = jnp.where(parity == 0, merged, partner_root)
    right_root = jnp.where(parity == 0, partner_root, merged)
    left_rows = lax.dynamic_slice_in_dim(left_root, parity * half_rows, half_rows, 0)
    left_times = jnp.dot(left_rows, full_grad, preferred_element_type=jnp.float32).astype(
        jnp.bfloat16
    )
    product = jnp.dot(left_times, right_root, preferred_element_type=jnp.float32)
    own_square = jnp.sum(product * product)
    other_square = swapped(own_square, "dev", 0)
    rms_scale = lax.rsqrt((own_square + other_square) / (block_width * block_width) + 1e-06)
    direction = (product * rms_scale).astype(jnp.bfloat16)

    fresh, direction = lax.optimization_barrier((fresh, direction))
    my_slots = lax.dynamic_slice_in_dim(refresh_stat, my_index * slot_count, slot_count, 0)
    fresh_roots = jnp.where(
        (my_slots >= 0)[:, None, None, None],
        fresh.transpose(1, 0, 2, 3),
        jnp.zeros((), jnp.bfloat16),
    ).reshape(slot_count, block_width, block_width)
    return (new_stat[None], merged[None], direction, fresh_roots)


def solution(mesh):
    in_specs = (
        P("dev", None),
        P("dev", None, None),
        P("dev", None, None),
        P("dev", None, None),
        P(),
        P(),
    )
    out_specs = (P("dev", None, None), P("dev", None, None), P("dev", None), P("dev", None, None))
    return jax.shard_map(
        per_device, mesh=mesh, in_specs=in_specs, out_specs=out_specs, check_vma=False
    )
```

```python
import jax
import jax.numpy as jnp
from jax import lax
from jax.experimental import pallas as pl
from jax.experimental.pallas import tpu as pltpu
from jax.sharding import PartitionSpec as P


ITERS = 2


decay_rate = 0.9


def swapped(shard, axis, bit):
    return lax.ppermute(shard, axis, [(i, i ^ 1 << bit) for i in range(lax.axis_size(axis))])


def spread(parts):
    return lax.all_to_all(parts, "dev", split_axis=0, concat_axis=0, tiled=True)


FIRST, OWN, SHARED, EXTRA = range(4)
EMPTY, PLAIN, HALVES, LATE = range(4)


def pick_kernel(kind_ref, row_ref, own_ref, *refs):
    tables, out_ref, sem = refs[:-3], refs[-3], refs[-1]
    width = out_ref.shape[2]
    half = width // 2

    def start(src, dst):
        pltpu.make_async_copy(src, dst, sem).start()

    def issue(item, carry):
        row, kind = row_ref[item], kind_ref[item]

        @pl.when(kind == FIRST)
        def _():
            start(tables[0].at[row], out_ref.at[item])

        @pl.when(kind != FIRST)
        def _():
            @pl.when(kind == OWN)
            def _():
                start(own_ref.at[row, :, pl.ds(0, width)], out_ref.at[item])

            @pl.when(kind == SHARED)
            def _():
                for core in range(2):
                    start(
                        own_ref.at[row // 2 * 2 + core, :, pl.ds(width, half)],
                        out_ref.at[item, :, pl.ds(core * half, half)],
                    )

            if len(tables) > 1:

                @pl.when(kind == EXTRA)
                def _():
                    for core in range(2):
                        start(
                            tables[1].at[row // 2 * 2 + core],
                            out_ref.at[item, :, pl.ds(core * half, half)],
                        )

        return carry

    lax.fori_loop(0, out_ref.shape[0], issue, 0, unroll=8)
    pltpu.make_async_copy(out_ref, out_ref, sem).wait()


def pick(kind, row, *tables):
    items, (_, piece_rows, width) = row.shape[0], tables[1].shape
    shape = jax.ShapeDtypeStruct((items, piece_rows, width), tables[0].dtype)
    anywhere = pl.BlockSpec(memory_space=pl.ANY)
    return pl.pallas_call(
        pick_kernel,
        out_shape=(shape, shape),
        in_specs=[pl.BlockSpec(memory_space=pltpu.SMEM)] * 2 + [anywhere] * len(tables),
        out_specs=(pl.BlockSpec(memory_space=pltpu.VMEM), anywhere),
        scratch_shapes=[pltpu.SemaphoreType.DMA],
        compiler_params=pltpu.CompilerParams(vmem_limit_bytes=8 * 1024 * 1024),
        cost_estimate=pl.CostEstimate(
            flops=4 * 1000 * 1000 * 1000, bytes_accessed=8 * 1000 * 1000, transcendentals=0
        ),
        name="pick",
    )(kind, row, *tables)


def route_kernel(row_ref, shared_row_ref, own_ref, out_ref, sem):
    half = out_ref.shape[2] // 3

    def issue(chip, carry):
        shared_row = shared_row_ref[chip]
        for core in range(2):
            item = chip * 2 + core
            pltpu.make_async_copy(
                own_ref.at[row_ref[item], :, pl.ds(0, 2 * half)],
                out_ref.at[item, :, pl.ds(0, 2 * half)],
                sem,
            ).start()
            pltpu.make_async_copy(
                own_ref.at[shared_row, :, pl.ds(core * half, half)],
                out_ref.at[item, :, pl.ds(2 * half, half)],
                sem,
            ).start()
        return carry

    lax.fori_loop(0, out_ref.shape[0] // 2, issue, 0, unroll=4)
    pltpu.make_async_copy(out_ref, out_ref, sem).wait()


def route(row, shared_row, own):
    return pl.pallas_call(
        route_kernel,
        out_shape=jax.ShapeDtypeStruct(own.shape, own.dtype),
        in_specs=[pl.BlockSpec(memory_space=pltpu.SMEM)] * 2
        + [pl.BlockSpec(memory_space=pl.ANY)],
        out_specs=pl.BlockSpec(memory_space=pltpu.VMEM),
        scratch_shapes=[pltpu.SemaphoreType.DMA],
        compiler_params=pltpu.CompilerParams(vmem_limit_bytes=8 * 1024 * 1024),
        cost_estimate=pl.CostEstimate(
            flops=4 * 1000 * 1000 * 1000, bytes_accessed=12 * 1000 * 1000, transcendentals=0
        ),
        name="route",
    )(row, shared_row, own)


def place_kernel(code_ref, got_ref, other_ref, late_ref, zero_ref, out_ref, held, zeros, sems):
    rows, width = late_ref.shape
    half, step = width // 2, rows // CHUNKS
    first, second, parity = code_ref[0], code_ref[1], code_ref[2]

    def side(core):
        return pl.ds(pl.multiple_of(core * half, half), half)

    def loads(slot, code, sem):
        into = held.at[slot]

        @pl.when(code == PLAIN)
        def _():
            pltpu.make_async_copy(got_ref.at[:, pl.ds(0, width)], into, sem).start()

        @pl.when(code == LATE)
        def _():
            pltpu.make_async_copy(late_ref, into, sem).start()

        @pl.when(code == HALVES)
        def _():
            pltpu.make_async_copy(
                got_ref.at[:, pl.ds(width, half)], into.at[:, side(parity)], sem
            ).start()
            pltpu.make_async_copy(other_ref, into.at[:, side(1 - parity)], sem).start()

    for slot, code in enumerate((first, second)):
        loads(slot, code, sems.at[slot])

    pltpu.make_async_copy(zero_ref, zeros, sems.at[3]).start()
    for slot, code in enumerate((first, second)):

        @pl.when(code != EMPTY)
        def _():
            pltpu.make_async_copy(late_ref, held.at[slot], sems.at[slot]).wait()
            pltpu.make_async_copy(held.at[slot], out_ref.at[slot], sems.at[2]).start()

    pltpu.make_async_copy(zero_ref, zeros, sems.at[3]).wait()
    for slot, code in enumerate((first, second)):

        @pl.when(code == EMPTY)
        def _():
            for chunk in range(CHUNKS):
                pltpu.make_async_copy(
                    zeros, out_ref.at[slot, pl.ds(chunk * step, step), :], sems.at[2]
                ).start()

    pltpu.make_async_copy(held, out_ref, sems.at[2]).wait()


def place(codes, got, other, late):
    rows, width = late.shape
    anywhere = pl.BlockSpec(memory_space=pl.ANY)
    return pl.pallas_call(
        place_kernel,
        out_shape=jax.ShapeDtypeStruct((2, rows, width), late.dtype),
        in_specs=[pl.BlockSpec(memory_space=pltpu.SMEM)] + [anywhere] * 4,
        out_specs=anywhere,
        scratch_shapes=[
            pltpu.VMEM((2, rows, width), late.dtype),
            pltpu.VMEM((rows // CHUNKS, width), late.dtype),
            pltpu.SemaphoreType.DMA((4,)),
        ],
        compiler_params=pltpu.CompilerParams(vmem_limit_bytes=8 * 1024 * 1024),
        name="place",
    )(codes, got, other, late, jnp.zeros((rows // CHUNKS, width), late.dtype))


CHUNKS = 4


def first_kernel(index_ref, stat_ref, pending_ref, first_ref, columns_ref, held, cut, sems):
    rows, width = first_ref.shape
    half, step = width // 2, rows // CHUNKS
    slot = jnp.where(stat_ref[index_ref[0] * 2] >= 0, 0, 1)
    other_half = pl.ds(pl.multiple_of((1 - index_ref[0] % 2) * half, half), half)
    moves = []
    for chunk in range(CHUNKS):
        part = pl.ds(chunk * step, step)
        moves.append((pending_ref.at[slot, part, :], held.at[part, :], first_ref.at[part, :]))
    moves.append((pending_ref.at[1, :, other_half], cut, columns_ref))
    loads = [
        pltpu.make_async_copy(src, mid, sems.at[0, pos]) for pos, (src, mid, dst) in enumerate(moves)
    ]
    stores = [
        pltpu.make_async_copy(mid, dst, sems.at[1, pos]) for pos, (src, mid, dst) in enumerate(moves)
    ]
    for load in loads:
        load.start()
    for load, store in zip(loads, stores):
        load.wait()
        store.start()
    for store in stores:
        store.wait()


def first_used(my_index, pending_stat, pending_roots):
    rows, width = pending_roots.shape[1:]
    kind = pending_roots.dtype
    anywhere = pl.BlockSpec(memory_space=pl.ANY)
    return pl.pallas_call(
        first_kernel,
        out_shape=(
            jax.ShapeDtypeStruct((rows, width), kind),
            jax.ShapeDtypeStruct((rows, width // 2), kind),
        ),
        in_specs=[pl.BlockSpec(memory_space=pltpu.SMEM)] * 2 + [anywhere],
        out_specs=(anywhere, anywhere),
        scratch_shapes=[
            pltpu.VMEM((rows, width), kind),
            pltpu.VMEM((rows, width // 2), kind),
            pltpu.SemaphoreType.DMA((2, CHUNKS + 1)),
        ],
        compiler_params=pltpu.CompilerParams(vmem_limit_bytes=8 * 1024 * 1024),
        name="first_used",
    )(my_index, pending_stat, pending_roots)


def poly_times(first, second):
    result = [0.0] * (len(first) + len(second) - 1)
    for left_pos in range(len(first)):
        for right_pos in range(len(second)):
            result[left_pos + right_pos] += first[left_pos] * second[right_pos]
    return result


def root_polynomial(iteration_count):
    x_poly = [1.0]
    m_poly = [0.0, 1.0]
    for _ in range(iteration_count):
        t_poly = [-value / 4.0 for value in m_poly]
        t_poly[0] += 5.0 / 4.0
        x_poly = poly_times(x_poly, t_poly)
        t_square = poly_times(t_poly, t_poly)
        m_poly = poly_times(poly_times(t_square, t_square), m_poly)
    return [float(value) for value in x_poly]


TILE = 256


def root_kernel(
    index_ref,
    pending_stat_ref,
    refresh_stat_ref,
    own_grad_ref,
    other_grad_ref,
    stat_ref,
    pending_ref,
    other_ref,
    new_ref,
    own_ref,
    grad_ref,
    grad,
    factor16,
    stat,
    scaled,
    scaled16,
    square,
    square16,
    cube16,
    upper16,
    root16,
    shared,
    sems,
):
    width = stat_ref.shape[0]
    half = width // 2
    tiles = width // TILE
    me = index_ref[0]
    parity = me % 2
    poly = root_polynomial(ITERS)

    def columns_of(step):
        return pl.ds(pl.multiple_of(step * TILE, TILE), TILE)

    def half_of(side):
        return pl.ds(pl.multiple_of(side * half, half), half)

    own_half = pltpu.make_async_copy(own_grad_ref, grad.at[half_of(parity), :], sems.at[0])
    other_half = pltpu.make_async_copy(other_grad_ref, grad.at[half_of(1 - parity), :], sems.at[1])
    statistic = pltpu.make_async_copy(stat_ref, stat, sems.at[2])
    grad_out = pltpu.make_async_copy(grad, grad_ref, sems.at[3])
    new_out = pltpu.make_async_copy(stat, new_ref, sems.at[4])
    second = pltpu.make_async_copy(pending_ref.at[1], root16, sems.at[5])
    shared_in = pltpu.make_async_copy(other_ref, shared, sems.at[6])
    shared_out = pltpu.make_async_copy(shared, own_ref.at[:, pl.ds(width, half)], sems.at[7])

    def root_out(step):
        return pltpu.make_async_copy(
            root16.at[:, columns_of(step)], own_ref.at[:, columns_of(step)], sems.at[8]
        )

    own_half.start()
    other_half.start()
    statistic.start()

    def look(item, found):
        entry = refresh_stat_ref[item]
        return found[0] | (entry == me), found[1] | (entry == me - parity)

    refreshed, core_refreshed = lax.fori_loop(
        0, refresh_stat_ref.shape[0], look, (jnp.bool_(False), jnp.bool_(False)), unroll=16
    )
    core = (me - parity) * 2
    core_shares = (
        core_refreshed & (pending_stat_ref[core] >= 0) & (pending_stat_ref[core + 1] >= 0)
    )
    from_other = core_shares == (parity == 1)

    @pl.when(from_other)
    def _():
        shared_in.start()

    @pl.when(jnp.logical_not(from_other))
    def _():
        pltpu.make_async_copy(
            pending_ref.at[1, :, half_of(parity)], shared, sems.at[6]
        ).start()

    @pl.when(jnp.logical_not(refreshed))
    def _():
        second.start()

    own_half.wait()
    other_half.wait()
    grad_out.start()

    @pl.when(parity == 0)
    def _():
        factor16[...] = grad[...]

    @pl.when(parity == 1)
    def _():
        @pl.loop(0, tiles)
        def _(step):
            columns = columns_of(step)
            factor16[columns, :] = jnp.transpose(grad[:, columns])

    statistic.wait()

    def update(step, trace):
        columns = columns_of(step)
        gram = lax.dot_general(
            factor16[...],
            factor16[columns, :],
            (((1,), (1,)), ((), ())),
            preferred_element_type=jnp.float32,
        )
        stat[:, columns] = decay_rate * stat[:, columns] + (1.0 - decay_rate) * gram
        block = stat[columns, columns]
        on_diagonal = lax.broadcasted_iota(jnp.int32, (TILE, TILE), 0) == lax.broadcasted_iota(
            jnp.int32, (TILE, TILE), 1
        )
        return trace + jnp.sum(jnp.where(on_diagonal, block, 0.0), axis=0, keepdims=True)

    diagonal = lax.fori_loop(0, tiles, update, jnp.zeros((1, TILE), jnp.float32))
    shared_in.wait()
    shared_out.start()

    @pl.when(jnp.logical_not(refreshed))
    def _():
        second.wait()
        new_out.start()
        for step in range(tiles):
            root_out(step).start()

    @pl.when(refreshed)
    def _():
        norm_scale = 2.0 * jnp.sum(diagonal, axis=1, keepdims=True) / width
        factor = lax.rsqrt(jnp.sqrt(norm_scale))

        @pl.loop(0, width // 128)
        def _(step):
            rows = pl.ds(pl.multiple_of(step * 128, 128), 128)
            part = stat[rows, :] / norm_scale
            scaled[rows, :] = part
            scaled16[rows, :] = part.astype(jnp.bfloat16)

        new_out.start()

        def identity(step):
            return (
                lax.broadcasted_iota(jnp.int32, (width, TILE), 0)
                == lax.broadcasted_iota(jnp.int32, (width, TILE), 1) + step * TILE
            )

        def dot(first, second):
            return jnp.dot(first, second, preferred_element_type=jnp.float32)

        @pl.loop(0, tiles)
        def _(step):
            columns = columns_of(step)
            tile = dot(scaled16[...], scaled16[:, columns])
            square[:, columns] = tile
            square16[:, columns] = tile.astype(jnp.bfloat16)

        @pl.loop(0, tiles)
        def _(step):
            columns = columns_of(step)
            cube = dot(square16[...], scaled16[:, columns])
            cube16[:, columns] = cube.astype(jnp.bfloat16)
            upper = (
                jnp.where(identity(step), poly[3], 0.0)
                + poly[4] * scaled[:, columns]
                + poly[5] * square[:, columns]
                + poly[6] * cube
            )
            upper16[:, columns] = upper.astype(jnp.bfloat16)

        @pl.loop(0, tiles)
        def _(step):
            columns = columns_of(step)
            total = dot(cube16[...], upper16[:, columns])
            total += (
                jnp.where(identity(step), poly[0], 0.0)
                + poly[1] * scaled[:, columns]
                + poly[2] * square[:, columns]
            )
            root16[:, columns] = (total * factor).astype(jnp.bfloat16)

            @pl.when(step > 0)
            def _():
                root_out(step - 1).start()

    grad_out.wait()
    new_out.wait()

    @pl.when(refreshed)
    def _():
        root_out(tiles - 1).start()

    shared_out.wait()
    pltpu.make_async_copy(root16, own_ref.at[:, pl.ds(0, width)], sems.at[8]).wait()


def updated_and_root(
    my_index, pending_stat, refresh_stat, own_grad, other_grad, statistic, pending_roots, columns
):
    width = statistic.shape[0]
    anywhere = pl.BlockSpec(memory_space=pl.ANY)
    plain = pltpu.VMEM((width, width), jnp.float32)
    short = pltpu.VMEM((width, width), jnp.bfloat16)
    return pl.pallas_call(
        root_kernel,
        out_shape=(
            jax.ShapeDtypeStruct((width, width), jnp.float32),
            jax.ShapeDtypeStruct((width, width + width // 2), jnp.bfloat16),
            jax.ShapeDtypeStruct((width, width), jnp.bfloat16),
        ),
        in_specs=[pl.BlockSpec(memory_space=pltpu.SMEM)] * 3 + [anywhere] * 5,
        out_specs=(anywhere,) * 3,
        scratch_shapes=[
            short,
            short,
            plain,
            plain,
            short,
            plain,
            short,
            short,
            short,
            short,
            pltpu.VMEM((width, width // 2), jnp.bfloat16),
            pltpu.SemaphoreType.DMA((9,)),
        ],
        compiler_params=pltpu.CompilerParams(vmem_limit_bytes=44 * 1024 * 1024),
        cost_estimate=pl.CostEstimate(
            flops=8 * width**3, bytes_accessed=17 * width * width, transcendentals=0
        ),
        name="root",
    )(
        my_index,
        pending_stat,
        refresh_stat,
        own_grad,
        other_grad,
        statistic,
        pending_roots,
        columns,
    )


def per_device(gradient, statistics, held_roots, pending_roots, pending_stat, refresh_stat):
    devices = lax.axis_size("dev")
    my_index = lax.axis_index("dev")
    parity = my_index % 2
    block_width = statistics.shape[1]
    piece_rows = block_width // devices
    slot_count = pending_roots.shape[0]
    half_rows = gradient.shape[0]
    half_columns = block_width // 2
    slot_total = pending_stat.shape[0]
    device_ids = jnp.arange(devices, dtype=jnp.int32)

    index_table = my_index.reshape(1)
    first_root, cut_columns = first_used(index_table, pending_stat, pending_roots)
    first_parts = spread(first_root.reshape(devices, piece_rows, block_width))
    other_columns = swapped(cut_columns, "dev", 0)

    new_stat, own_matrix, full_grad = updated_and_root(
        index_table,
        pending_stat,
        refresh_stat,
        gradient,
        swapped(gradient, "dev", 0),
        statistics[0],
        pending_roots,
        other_columns,
    )
    root_parts = spread(own_matrix.reshape(devices, piece_rows, block_width + half_columns))

    has_first = pending_stat.reshape(devices, slot_count)[:, 0] >= 0
    has_second = has_first & (pending_stat.reshape(devices, slot_count)[:, 1] >= 0)
    refreshed = jnp.any(refresh_stat[None, :] == device_ids[:, None], axis=1)
    sharing_pairs = (has_second & refreshed).reshape(devices // 2, 2)
    unplaced = jnp.any(sharing_pairs[:, 0] & sharing_pairs[:, 1])
    slot_ids = jnp.arange(slot_total, dtype=jnp.int32)
    slot_match = pending_stat[None, :] == device_ids[:, None]
    found = jnp.any(slot_match, axis=1)
    slot_of = jnp.sum(jnp.where(slot_match, slot_ids[None, :], 0), axis=1)
    is_second = jnp.any(
        slot_match & (slot_ids % slot_count == 1) & jnp.repeat(has_first, slot_count), axis=1
    )
    is_shared = jnp.any(slot_match & jnp.repeat(refreshed, slot_count), axis=1)
    is_extra = jnp.any(
        slot_match
        & (slot_ids // slot_count % 2 == 1)
        & jnp.repeat(sharing_pairs[:, 0], 2 * slot_count),
        axis=1,
    )
    shared_kind = jnp.where(is_extra, EXTRA, SHARED)
    kind = jnp.where(is_second, jnp.where(is_shared, shared_kind, OWN), FIRST)

    wanted = refresh_stat.reshape(devices, slot_count)
    wants_two = (wanted[:, 0] >= 0) & (wanted[:, 1] >= 0)
    two_pairs = wants_two.reshape(devices // 2, 2)
    second_pairs = jnp.maximum(wanted[:, 1], 0).reshape(devices // 2, 2)
    first_wanted = jnp.maximum(jnp.where(wanted[:, 0] >= 0, wanted[:, 0], wanted[:, 1]), 0)
    shared_wanted = jnp.where(two_pairs[:, 0], second_pairs[:, 0], second_pairs[:, 1])
    fourth = two_pairs[:, 0] & two_pairs[:, 1]
    found_pairs = found.reshape(devices // 2, 2)
    unrouted = jnp.any(fourth & found_pairs[:, 0] & found_pairs[:, 1])
    carries = (
        jnp.repeat(fourth, 2)
        & jnp.logical_not(found)
        & ((device_ids % 2 == 1) | jnp.repeat(found_pairs[:, 1], 2))
    )
    kind = jnp.where(carries, OWN, kind).astype(jnp.int32)
    source = jnp.where(carries, jnp.repeat(second_pairs[:, 1], 2), slot_of // slot_count)

    def choose(more_pending, more_fresh):
        def run():
            tables = [root_parts, first_parts]
            if more_pending:
                columns = jnp.where(
                    parity == 0, other_columns, pending_roots[1][:, half_columns:]
                )
                tables.append(spread(columns.reshape(devices, piece_rows, half_columns)))
            chosen, spare = pick(kind, source, *tables)
            if more_fresh:
                late, _ = pick(
                    jnp.full((devices,), OWN, jnp.int32), jnp.maximum(wanted[:, 1], 0), *tables[:2]
                )
                spare = spread(late)
            return chosen, spare

        return run

    chosen, spare = lax.switch(
        unplaced + 2 * unrouted.astype(jnp.int32),
        [choose(more % 2 == 1, more // 2 == 1) for more in range(4)],
    )
    chosen, spare = lax.optimization_barrier((chosen, spare))
    returned = spread(chosen).reshape(block_width, block_width)
    routed = route(first_wanted, shared_wanted, root_parts)
    fresh = spread(routed).reshape(block_width, block_width + half_columns)

    my_found = jnp.any(pending_stat == my_index)
    partner_found = jnp.any(pending_stat == my_index + 1 - 2 * parity)
    merged = jnp.where(my_found, returned, held_roots[0])
    late = jnp.where(
        my_found,
        jnp.where(
            partner_found, spare.reshape(block_width, block_width), swapped(returned, "dev", 0)
        ),
        returned,
    )

    partner_root = swapped(merged, "dev", 0)
    left_root = jnp.where(parity == 0, merged, partner_root)
    right_root = jnp.where(parity == 0, partner_root, merged)
    left_rows = lax.dynamic_slice_in_dim(left_root, parity * half_rows, half_rows, 0)
    left_times = jnp.dot(left_rows, full_grad, preferred_element_type=jnp.float32).astype(
        jnp.bfloat16
    )
    product = jnp.dot(left_times, right_root, preferred_element_type=jnp.float32)
    own_square = jnp.sum(product * product)
    other_square = swapped(own_square, "dev", 0)
    rms_scale = lax.rsqrt((own_square + other_square) / (block_width * block_width) + 1e-06)
    direction = (product * rms_scale).astype(jnp.bfloat16)

    my_slots = lax.dynamic_slice_in_dim(refresh_stat, my_index * slot_count, slot_count, 0)
    core_slots = lax.dynamic_slice_in_dim(
        refresh_stat, (my_index - parity) * slot_count, slot_count, 0
    )
    is_fourth = (parity == 1) & jnp.all(core_slots >= 0)
    doubled = jnp.where(is_fourth, LATE, HALVES)
    codes = jnp.stack(
        [
            jnp.where(my_slots[0] >= 0, PLAIN, EMPTY),
            jnp.where(my_slots[1] >= 0, jnp.where(my_slots[0] >= 0, doubled, PLAIN), EMPTY),
            parity,
        ]
    ).astype(jnp.int32)
    fresh, direction, codes, late = lax.optimization_barrier((fresh, direction, codes, late))
    fresh_roots = place(codes, fresh, swapped(fresh[:, block_width:], "dev", 0), late)
    return (new_stat[None], merged[None], direction, fresh_roots)


def solution(mesh):
    in_specs = (
        P("dev", None),
        P("dev", None, None),
        P("dev", None, None),
        P("dev", None, None),
        P(),
        P(),
    )
    out_specs = (P("dev", None, None), P("dev", None, None), P("dev", None), P("dev", None, None))
    return jax.shard_map(
        per_device, mesh=mesh, in_specs=in_specs, out_specs=out_specs, check_vma=False
    )
```

```python
import jax
import jax.numpy as jnp
from jax import lax
from jax.experimental import pallas as pl
from jax.experimental.pallas import tpu as pltpu
from jax.sharding import PartitionSpec as P


ITERS = 2


decay_rate = 0.9


def swapped(shard, axis, bit):
    return lax.ppermute(shard, axis, [(i, i ^ 1 << bit) for i in range(lax.axis_size(axis))])


def spread(parts):
    return lax.all_to_all(parts, "dev", split_axis=0, concat_axis=0, tiled=True)


FIRST, OWN, SHARED, EXTRA = range(4)
EMPTY, PLAIN, HALVES, LATE = range(4)


def pick_kernel(kind_ref, row_ref, own_ref, *refs):
    tables, out_ref, sem = refs[:-3], refs[-3], refs[-1]
    width = out_ref.shape[2]
    half = width // 2

    def start(src, dst):
        pltpu.make_async_copy(src, dst, sem).start()

    def issue(item, carry):
        row, kind = row_ref[item], kind_ref[item]

        @pl.when(kind == FIRST)
        def _():
            start(tables[0].at[row], out_ref.at[item])

        @pl.when(kind != FIRST)
        def _():
            @pl.when(kind == OWN)
            def _():
                start(own_ref.at[row, :, pl.ds(0, width)], out_ref.at[item])

            @pl.when(kind == SHARED)
            def _():
                for core in range(2):
                    start(
                        own_ref.at[row // 2 * 2 + core, :, pl.ds(width, half)],
                        out_ref.at[item, :, pl.ds(core * half, half)],
                    )

            if len(tables) > 1:

                @pl.when(kind == EXTRA)
                def _():
                    for core in range(2):
                        start(
                            tables[1].at[row // 2 * 2 + core],
                            out_ref.at[item, :, pl.ds(core * half, half)],
                        )

        return carry

    lax.fori_loop(0, out_ref.shape[0], issue, 0, unroll=8)
    pltpu.make_async_copy(out_ref, out_ref, sem).wait()


def pick(kind, row, *tables):
    items, (_, piece_rows, width) = row.shape[0], tables[1].shape
    shape = jax.ShapeDtypeStruct((items, piece_rows, width), tables[0].dtype)
    anywhere = pl.BlockSpec(memory_space=pl.ANY)
    return pl.pallas_call(
        pick_kernel,
        out_shape=(shape, shape),
        in_specs=[pl.BlockSpec(memory_space=pltpu.SMEM)] * 2 + [anywhere] * len(tables),
        out_specs=(pl.BlockSpec(memory_space=pltpu.VMEM), anywhere),
        scratch_shapes=[pltpu.SemaphoreType.DMA],
        compiler_params=pltpu.CompilerParams(vmem_limit_bytes=8 * 1024 * 1024),
        cost_estimate=pl.CostEstimate(
            flops=4 * 1000 * 1000 * 1000, bytes_accessed=8 * 1000 * 1000, transcendentals=0
        ),
        name="pick",
    )(kind, row, *tables)


def route_kernel(row_ref, shared_row_ref, own_ref, out_ref, sem):
    half = out_ref.shape[2] // 3

    def issue(chip, carry):
        shared_row = shared_row_ref[chip]
        for core in range(2):
            item = chip * 2 + core
            pltpu.make_async_copy(
                own_ref.at[row_ref[item], :, pl.ds(0, 2 * half)],
                out_ref.at[item, :, pl.ds(0, 2 * half)],
                sem,
            ).start()
            pltpu.make_async_copy(
                own_ref.at[shared_row, :, pl.ds(core * half, half)],
                out_ref.at[item, :, pl.ds(2 * half, half)],
                sem,
            ).start()
        return carry

    lax.fori_loop(0, out_ref.shape[0] // 2, issue, 0, unroll=4)
    pltpu.make_async_copy(out_ref, out_ref, sem).wait()


def route(row, shared_row, own):
    return pl.pallas_call(
        route_kernel,
        out_shape=jax.ShapeDtypeStruct(own.shape, own.dtype),
        in_specs=[pl.BlockSpec(memory_space=pltpu.SMEM)] * 2
        + [pl.BlockSpec(memory_space=pl.ANY)],
        out_specs=pl.BlockSpec(memory_space=pltpu.VMEM),
        scratch_shapes=[pltpu.SemaphoreType.DMA],
        compiler_params=pltpu.CompilerParams(vmem_limit_bytes=8 * 1024 * 1024),
        cost_estimate=pl.CostEstimate(
            flops=4 * 1000 * 1000 * 1000, bytes_accessed=12 * 1000 * 1000, transcendentals=0
        ),
        name="route",
    )(row, shared_row, own)


def place_kernel(code_ref, got_ref, other_ref, late_ref, zero_ref, out_ref, held, zeros, sems):
    rows, width = late_ref.shape
    half, step = width // 2, rows // CHUNKS
    first, second, parity = code_ref[0], code_ref[1], code_ref[2]

    def side(core):
        return pl.ds(pl.multiple_of(core * half, half), half)

    def loads(slot, code, sem):
        into = held.at[slot]

        @pl.when(code == PLAIN)
        def _():
            pltpu.make_async_copy(got_ref.at[:, pl.ds(0, width)], into, sem).start()

        @pl.when(code == LATE)
        def _():
            pltpu.make_async_copy(late_ref, into, sem).start()

        @pl.when(code == HALVES)
        def _():
            pltpu.make_async_copy(
                got_ref.at[:, pl.ds(width, half)], into.at[:, side(parity)], sem
            ).start()
            pltpu.make_async_copy(other_ref, into.at[:, side(1 - parity)], sem).start()

    for slot, code in enumerate((first, second)):
        loads(slot, code, sems.at[slot])

    pltpu.make_async_copy(zero_ref, zeros, sems.at[3]).start()
    for slot, code in enumerate((first, second)):

        @pl.when(code != EMPTY)
        def _():
            pltpu.make_async_copy(late_ref, held.at[slot], sems.at[slot]).wait()
            pltpu.make_async_copy(held.at[slot], out_ref.at[slot], sems.at[2]).start()

    pltpu.make_async_copy(zero_ref, zeros, sems.at[3]).wait()
    for slot, code in enumerate((first, second)):

        @pl.when(code == EMPTY)
        def _():
            for chunk in range(CHUNKS):
                pltpu.make_async_copy(
                    zeros, out_ref.at[slot, pl.ds(chunk * step, step), :], sems.at[2]
                ).start()

    pltpu.make_async_copy(held, out_ref, sems.at[2]).wait()


def place(codes, got, other, late):
    rows, width = late.shape
    anywhere = pl.BlockSpec(memory_space=pl.ANY)
    return pl.pallas_call(
        place_kernel,
        out_shape=jax.ShapeDtypeStruct((2, rows, width), late.dtype),
        in_specs=[pl.BlockSpec(memory_space=pltpu.SMEM)] + [anywhere] * 4,
        out_specs=anywhere,
        scratch_shapes=[
            pltpu.VMEM((2, rows, width), late.dtype),
            pltpu.VMEM((rows // CHUNKS, width), late.dtype),
            pltpu.SemaphoreType.DMA((4,)),
        ],
        compiler_params=pltpu.CompilerParams(vmem_limit_bytes=8 * 1024 * 1024),
        name="place",
    )(codes, got, other, late, jnp.zeros((rows // CHUNKS, width), late.dtype))


CHUNKS = 4


def first_kernel(index_ref, stat_ref, pending_ref, first_ref, held, sems):
    step = first_ref.shape[0] // CHUNKS
    slot = jnp.where(stat_ref[index_ref[0] * 2] >= 0, 0, 1)
    parts = [pl.ds(chunk * step, step) for chunk in range(CHUNKS)]
    loads = [
        pltpu.make_async_copy(pending_ref.at[slot, part, :], held.at[part, :], sems.at[0, pos])
        for pos, part in enumerate(parts)
    ]
    stores = [
        pltpu.make_async_copy(held.at[part, :], first_ref.at[part, :], sems.at[1, pos])
        for pos, part in enumerate(parts)
    ]
    for load in loads:
        load.start()
    for load, store in zip(loads, stores):
        load.wait()
        store.start()
    for store in stores:
        store.wait()


def first_used(my_index, pending_stat, pending_roots):
    shape, kind = pending_roots.shape[1:], pending_roots.dtype
    anywhere = pl.BlockSpec(memory_space=pl.ANY)
    return pl.pallas_call(
        first_kernel,
        out_shape=jax.ShapeDtypeStruct(shape, kind),
        in_specs=[pl.BlockSpec(memory_space=pltpu.SMEM)] * 2 + [anywhere],
        out_specs=anywhere,
        scratch_shapes=[pltpu.VMEM(shape, kind), pltpu.SemaphoreType.DMA((2, CHUNKS))],
        compiler_params=pltpu.CompilerParams(vmem_limit_bytes=8 * 1024 * 1024),
        name="first_used",
    )(my_index, pending_stat, pending_roots)


def poly_times(first, second):
    result = [0.0] * (len(first) + len(second) - 1)
    for left_pos in range(len(first)):
        for right_pos in range(len(second)):
            result[left_pos + right_pos] += first[left_pos] * second[right_pos]
    return result


def root_polynomial(iteration_count):
    x_poly = [1.0]
    m_poly = [0.0, 1.0]
    for _ in range(iteration_count):
        t_poly = [-value / 4.0 for value in m_poly]
        t_poly[0] += 5.0 / 4.0
        x_poly = poly_times(x_poly, t_poly)
        t_square = poly_times(t_poly, t_poly)
        m_poly = poly_times(poly_times(t_square, t_square), m_poly)
    return [float(value) for value in x_poly]


TILE = 256


def root_kernel(
    index_ref,
    pending_stat_ref,
    refresh_stat_ref,
    own_grad_ref,
    other_grad_ref,
    stat_ref,
    pending_ref,
    other_ref,
    new_ref,
    own_ref,
    grad_ref,
    grad,
    factor16,
    stat,
    scaled,
    scaled16,
    square,
    square16,
    cube16,
    upper16,
    root16,
    shared,
    sems,
):
    width = stat_ref.shape[0]
    half = width // 2
    tiles = width // TILE
    me = index_ref[0]
    parity = me % 2
    poly = root_polynomial(ITERS)

    def columns_of(step):
        return pl.ds(pl.multiple_of(step * TILE, TILE), TILE)

    def half_of(side):
        return pl.ds(pl.multiple_of(side * half, half), half)

    own_half = pltpu.make_async_copy(own_grad_ref, grad.at[half_of(parity), :], sems.at[0])
    other_half = pltpu.make_async_copy(other_grad_ref, grad.at[half_of(1 - parity), :], sems.at[1])
    statistic = pltpu.make_async_copy(stat_ref, stat, sems.at[2])
    grad_out = pltpu.make_async_copy(grad, grad_ref, sems.at[3])
    new_out = pltpu.make_async_copy(stat, new_ref, sems.at[4])
    second = pltpu.make_async_copy(pending_ref.at[1], root16, sems.at[5])
    shared_in = pltpu.make_async_copy(other_ref, shared, sems.at[6])
    shared_out = pltpu.make_async_copy(shared, own_ref.at[:, pl.ds(width, half)], sems.at[7])

    def root_out(step):
        return pltpu.make_async_copy(
            root16.at[:, columns_of(step)], own_ref.at[:, columns_of(step)], sems.at[8]
        )

    own_half.start()
    other_half.start()
    statistic.start()

    def look(item, found):
        entry = refresh_stat_ref[item]
        return found[0] | (entry == me), found[1] | (entry == me - parity)

    refreshed, core_refreshed = lax.fori_loop(
        0, refresh_stat_ref.shape[0], look, (jnp.bool_(False), jnp.bool_(False)), unroll=16
    )
    core = (me - parity) * 2
    core_shares = (
        core_refreshed & (pending_stat_ref[core] >= 0) & (pending_stat_ref[core + 1] >= 0)
    )
    from_other = core_shares == (parity == 1)

    @pl.when(from_other)
    def _():
        shared_in.start()

    @pl.when(jnp.logical_not(from_other))
    def _():
        pltpu.make_async_copy(
            pending_ref.at[1, :, half_of(parity)], shared, sems.at[6]
        ).start()

    @pl.when(jnp.logical_not(refreshed))
    def _():
        second.start()

    own_half.wait()
    other_half.wait()
    grad_out.start()

    @pl.when(parity == 0)
    def _():
        factor16[...] = grad[...]

    @pl.when(parity == 1)
    def _():
        @pl.loop(0, tiles)
        def _(step):
            columns = columns_of(step)
            factor16[columns, :] = jnp.transpose(grad[:, columns])

    statistic.wait()

    def update(step, trace):
        columns = columns_of(step)
        gram = lax.dot_general(
            factor16[...],
            factor16[columns, :],
            (((1,), (1,)), ((), ())),
            preferred_element_type=jnp.float32,
        )
        stat[:, columns] = decay_rate * stat[:, columns] + (1.0 - decay_rate) * gram
        block = stat[columns, columns]
        on_diagonal = lax.broadcasted_iota(jnp.int32, (TILE, TILE), 0) == lax.broadcasted_iota(
            jnp.int32, (TILE, TILE), 1
        )
        return trace + jnp.sum(jnp.where(on_diagonal, block, 0.0), axis=0, keepdims=True)

    diagonal = lax.fori_loop(0, tiles, update, jnp.zeros((1, TILE), jnp.float32))
    shared_in.wait()
    shared_out.start()

    @pl.when(jnp.logical_not(refreshed))
    def _():
        second.wait()
        new_out.start()
        for step in range(tiles):
            root_out(step).start()

    @pl.when(refreshed)
    def _():
        norm_scale = 2.0 * jnp.sum(diagonal, axis=1, keepdims=True) / width
        factor = lax.rsqrt(jnp.sqrt(norm_scale))

        @pl.loop(0, width // 128)
        def _(step):
            rows = pl.ds(pl.multiple_of(step * 128, 128), 128)
            part = stat[rows, :] / norm_scale
            scaled[rows, :] = part
            scaled16[rows, :] = part.astype(jnp.bfloat16)

        new_out.start()

        def identity(step):
            return (
                lax.broadcasted_iota(jnp.int32, (width, TILE), 0)
                == lax.broadcasted_iota(jnp.int32, (width, TILE), 1) + step * TILE
            )

        def dot(first, second):
            return jnp.dot(first, second, preferred_element_type=jnp.float32)

        @pl.loop(0, tiles)
        def _(step):
            columns = columns_of(step)
            tile = dot(scaled16[...], scaled16[:, columns])
            square[:, columns] = tile
            square16[:, columns] = tile.astype(jnp.bfloat16)

        @pl.loop(0, tiles)
        def _(step):
            columns = columns_of(step)
            cube = dot(square16[...], scaled16[:, columns])
            cube16[:, columns] = cube.astype(jnp.bfloat16)
            upper = (
                jnp.where(identity(step), poly[3], 0.0)
                + poly[4] * scaled[:, columns]
                + poly[5] * square[:, columns]
                + poly[6] * cube
            )
            upper16[:, columns] = upper.astype(jnp.bfloat16)

        @pl.loop(0, tiles)
        def _(step):
            columns = columns_of(step)
            total = dot(cube16[...], upper16[:, columns])
            total += (
                jnp.where(identity(step), poly[0], 0.0)
                + poly[1] * scaled[:, columns]
                + poly[2] * square[:, columns]
            )
            root16[:, columns] = (total * factor).astype(jnp.bfloat16)

            @pl.when(step > 0)
            def _():
                root_out(step - 1).start()

    grad_out.wait()
    new_out.wait()

    @pl.when(refreshed)
    def _():
        root_out(tiles - 1).start()

    shared_out.wait()
    pltpu.make_async_copy(root16, own_ref.at[:, pl.ds(0, width)], sems.at[8]).wait()


def updated_and_root(
    my_index, pending_stat, refresh_stat, own_grad, other_grad, statistic, pending_roots, columns
):
    width = statistic.shape[0]
    anywhere = pl.BlockSpec(memory_space=pl.ANY)
    plain = pltpu.VMEM((width, width), jnp.float32)
    short = pltpu.VMEM((width, width), jnp.bfloat16)
    return pl.pallas_call(
        root_kernel,
        out_shape=(
            jax.ShapeDtypeStruct((width, width), jnp.float32),
            jax.ShapeDtypeStruct((width, width + width // 2), jnp.bfloat16),
            jax.ShapeDtypeStruct((width, width), jnp.bfloat16),
        ),
        in_specs=[pl.BlockSpec(memory_space=pltpu.SMEM)] * 3 + [anywhere] * 5,
        out_specs=(anywhere,) * 3,
        scratch_shapes=[
            short,
            short,
            plain,
            plain,
            short,
            plain,
            short,
            short,
            short,
            short,
            pltpu.VMEM((width, width // 2), jnp.bfloat16),
            pltpu.SemaphoreType.DMA((9,)),
        ],
        compiler_params=pltpu.CompilerParams(vmem_limit_bytes=44 * 1024 * 1024),
        cost_estimate=pl.CostEstimate(
            flops=8 * width**3, bytes_accessed=17 * width * width, transcendentals=0
        ),
        name="root",
    )(
        my_index,
        pending_stat,
        refresh_stat,
        own_grad,
        other_grad,
        statistic,
        pending_roots,
        columns,
    )


def per_device(gradient, statistics, held_roots, pending_roots, pending_stat, refresh_stat):
    devices = lax.axis_size("dev")
    my_index = lax.axis_index("dev")
    parity = my_index % 2
    block_width = statistics.shape[1]
    piece_rows = block_width // devices
    slot_count = pending_roots.shape[0]
    half_rows = gradient.shape[0]
    half_columns = block_width // 2
    slot_total = pending_stat.shape[0]
    device_ids = jnp.arange(devices, dtype=jnp.int32)

    index_table = my_index.reshape(1)
    first_root = first_used(index_table, pending_stat, pending_roots)
    first_parts = spread(first_root.reshape(devices, piece_rows, block_width))
    cut_columns = lax.dynamic_slice(
        pending_roots, (1, 0, (1 - parity) * half_columns), (1, block_width, half_columns)
    )[0]
    other_columns = swapped(cut_columns, "dev", 0)

    new_stat, own_matrix, full_grad = updated_and_root(
        index_table,
        pending_stat,
        refresh_stat,
        gradient,
        swapped(gradient, "dev", 0),
        statistics[0],
        pending_roots,
        other_columns,
    )
    root_parts = spread(own_matrix.reshape(devices, piece_rows, block_width + half_columns))

    has_first = pending_stat.reshape(devices, slot_count)[:, 0] >= 0
    has_second = has_first & (pending_stat.reshape(devices, slot_count)[:, 1] >= 0)
    refreshed = jnp.any(refresh_stat[None, :] == device_ids[:, None], axis=1)
    sharing_pairs = (has_second & refreshed).reshape(devices // 2, 2)
    unplaced = jnp.any(sharing_pairs[:, 0] & sharing_pairs[:, 1])
    slot_ids = jnp.arange(slot_total, dtype=jnp.int32)
    slot_match = pending_stat[None, :] == device_ids[:, None]
    found = jnp.any(slot_match, axis=1)
    slot_of = jnp.sum(jnp.where(slot_match, slot_ids[None, :], 0), axis=1)
    is_second = jnp.any(
        slot_match & (slot_ids % slot_count == 1) & jnp.repeat(has_first, slot_count), axis=1
    )
    is_shared = jnp.any(slot_match & jnp.repeat(refreshed, slot_count), axis=1)
    is_extra = jnp.any(
        slot_match
        & (slot_ids // slot_count % 2 == 1)
        & jnp.repeat(sharing_pairs[:, 0], 2 * slot_count),
        axis=1,
    )
    shared_kind = jnp.where(is_extra, EXTRA, SHARED)
    kind = jnp.where(is_second, jnp.where(is_shared, shared_kind, OWN), FIRST)

    wanted = refresh_stat.reshape(devices, slot_count)
    wants_two = (wanted[:, 0] >= 0) & (wanted[:, 1] >= 0)
    two_pairs = wants_two.reshape(devices // 2, 2)
    second_pairs = jnp.maximum(wanted[:, 1], 0).reshape(devices // 2, 2)
    first_wanted = jnp.maximum(jnp.where(wanted[:, 0] >= 0, wanted[:, 0], wanted[:, 1]), 0)
    shared_wanted = jnp.where(two_pairs[:, 0], second_pairs[:, 0], second_pairs[:, 1])
    fourth = two_pairs[:, 0] & two_pairs[:, 1]
    found_pairs = found.reshape(devices // 2, 2)
    unrouted = jnp.any(fourth & found_pairs[:, 0] & found_pairs[:, 1])
    carries = (
        jnp.repeat(fourth, 2)
        & jnp.logical_not(found)
        & ((device_ids % 2 == 1) | jnp.repeat(found_pairs[:, 1], 2))
    )
    kind = jnp.where(carries, OWN, kind).astype(jnp.int32)
    source = jnp.where(carries, jnp.repeat(second_pairs[:, 1], 2), slot_of // slot_count)

    def choose(more_pending, more_fresh):
        def run():
            tables = [root_parts, first_parts]
            if more_pending:
                columns = jnp.where(
                    parity == 0, other_columns, pending_roots[1][:, half_columns:]
                )
                tables.append(spread(columns.reshape(devices, piece_rows, half_columns)))
            chosen, spare = pick(kind, source, *tables)
            if more_fresh:
                late, _ = pick(
                    jnp.full((devices,), OWN, jnp.int32), jnp.maximum(wanted[:, 1], 0), *tables[:2]
                )
                spare = spread(late)
            return chosen, spare

        return run

    chosen, spare = lax.switch(
        unplaced + 2 * unrouted.astype(jnp.int32),
        [choose(more % 2 == 1, more // 2 == 1) for more in range(4)],
    )
    chosen, spare = lax.optimization_barrier((chosen, spare))
    returned = spread(chosen).reshape(block_width, block_width)
    routed = route(first_wanted, shared_wanted, root_parts)
    fresh = spread(routed).reshape(block_width, block_width + half_columns)

    my_found = jnp.any(pending_stat == my_index)
    partner_found = jnp.any(pending_stat == my_index + 1 - 2 * parity)
    other_returned = swapped(returned, "dev", 0)
    merged = lax.optimization_barrier(jnp.where(my_found, returned, held_roots[0]))
    late = jnp.where(
        my_found,
        jnp.where(partner_found, spare.reshape(block_width, block_width), other_returned),
        returned,
    )

    partner_root = swapped(merged, "dev", 0)
    left_root = jnp.where(parity == 0, merged, partner_root)
    right_root = jnp.where(parity == 0, partner_root, merged)
    left_rows = lax.dynamic_slice_in_dim(left_root, parity * half_rows, half_rows, 0)
    left_times = jnp.dot(left_rows, full_grad, preferred_element_type=jnp.float32).astype(
        jnp.bfloat16
    )
    product = jnp.dot(left_times, right_root, preferred_element_type=jnp.float32)
    own_square = jnp.sum(product * product)
    other_square = swapped(own_square, "dev", 0)
    rms_scale = lax.rsqrt((own_square + other_square) / (block_width * block_width) + 1e-06)
    direction = (product * rms_scale).astype(jnp.bfloat16)

    my_slots = lax.dynamic_slice_in_dim(refresh_stat, my_index * slot_count, slot_count, 0)
    core_slots = lax.dynamic_slice_in_dim(
        refresh_stat, (my_index - parity) * slot_count, slot_count, 0
    )
    is_fourth = (parity == 1) & jnp.all(core_slots >= 0)
    doubled = jnp.where(is_fourth, LATE, HALVES)
    codes = jnp.stack(
        [
            jnp.where(my_slots[0] >= 0, PLAIN, EMPTY),
            jnp.where(my_slots[1] >= 0, jnp.where(my_slots[0] >= 0, doubled, PLAIN), EMPTY),
            parity,
        ]
    ).astype(jnp.int32)
    fresh, direction, codes, late = lax.optimization_barrier((fresh, direction, codes, late))
    fresh_roots = place(codes, fresh, swapped(fresh[:, block_width:], "dev", 0), late)
    return (new_stat[None], merged[None], direction, fresh_roots)


def solution(mesh):
    in_specs = (
        P("dev", None),
        P("dev", None, None),
        P("dev", None, None),
        P("dev", None, None),
        P(),
        P(),
    )
    out_specs = (P("dev", None, None), P("dev", None, None), P("dev", None), P("dev", None, None))
    return jax.shard_map(
        per_device, mesh=mesh, in_specs=in_specs, out_specs=out_specs, check_vma=False
    )
```

```python
import jax
import jax.numpy as jnp
from jax import lax
from jax.experimental import pallas as pl
from jax.experimental.pallas import tpu as pltpu
from jax.sharding import PartitionSpec as P


ITERS = 2


decay_rate = 0.9


def swapped(shard, axis, bit):
    return lax.ppermute(shard, axis, [(i, i ^ 1 << bit) for i in range(lax.axis_size(axis))])


def spread(parts):
    return lax.all_to_all(parts, "dev", split_axis=0, concat_axis=0, tiled=True)


FIRST, OWN, SHARED, EXTRA = range(4)
EMPTY, PLAIN, HALVES, LATE = range(4)


def gather_kernel(row_ref, table_ref, out_ref, sem):
    def issue(item, carry):
        pltpu.make_async_copy(table_ref.at[row_ref[item]], out_ref.at[item], sem).start()
        return carry

    lax.fori_loop(0, out_ref.shape[0], issue, 0, unroll=8)
    pltpu.make_async_copy(out_ref, out_ref, sem).wait()


def gather(row, table):
    return pl.pallas_call(
        gather_kernel,
        out_shape=jax.ShapeDtypeStruct(table.shape, table.dtype),
        in_specs=[
            pl.BlockSpec(memory_space=pltpu.SMEM),
            pl.BlockSpec(memory_space=pl.ANY),
        ],
        out_specs=pl.BlockSpec(memory_space=pltpu.VMEM),
        scratch_shapes=[pltpu.SemaphoreType.DMA],
        compiler_params=pltpu.CompilerParams(vmem_limit_bytes=8 * 1024 * 1024),
        cost_estimate=pl.CostEstimate(
            flops=4 * 1000 * 1000 * 1000, bytes_accessed=8 * 1000 * 1000, transcendentals=0
        ),
        name="gather",
    )(row, table)


def pick_kernel(kind_ref, row_ref, base_ref, own_ref, *refs):
    tables, out_ref, base_sem, sems = refs[:-4], refs[-4], refs[-2], refs[-1]
    items, _, width = out_ref.shape
    half = width // 2
    base = pltpu.make_async_copy(base_ref, out_ref, base_sem)
    base.start()
    base.wait()

    def issue(item, carry):
        row, kind = row_ref[item], kind_ref[item]

        def start(src, dst):
            pltpu.make_async_copy(src, dst, sems.at[item]).start()

        @pl.when(kind != FIRST)
        def _():
            @pl.when(kind == OWN)
            def _():
                start(own_ref.at[row, :, pl.ds(0, width)], out_ref.at[item])

            @pl.when(kind == SHARED)
            def _():
                for core in range(2):
                    start(
                        own_ref.at[row // 2 * 2 + core, :, pl.ds(width, half)],
                        out_ref.at[item, :, pl.ds(core * half, half)],
                    )

            if tables:

                @pl.when(kind == EXTRA)
                def _():
                    for core in range(2):
                        start(
                            tables[0].at[row // 2 * 2 + core],
                            out_ref.at[item, :, pl.ds(core * half, half)],
                        )

        return carry

    def finish(item, carry):
        @pl.when(kind_ref[item] != FIRST)
        def _():
            pltpu.make_async_copy(out_ref.at[item], out_ref.at[item], sems.at[item]).wait()

        return carry

    lax.fori_loop(0, items, issue, 0, unroll=8)
    lax.fori_loop(0, items, finish, 0, unroll=8)


def pick(kind, row, base, *tables):
    shape = jax.ShapeDtypeStruct(base.shape, base.dtype)
    anywhere = pl.BlockSpec(memory_space=pl.ANY)
    return pl.pallas_call(
        pick_kernel,
        out_shape=(shape, shape),
        in_specs=[pl.BlockSpec(memory_space=pltpu.SMEM)] * 2 + [anywhere] * (1 + len(tables)),
        out_specs=(pl.BlockSpec(memory_space=pltpu.VMEM), anywhere),
        scratch_shapes=[
            pltpu.SemaphoreType.DMA,
            pltpu.SemaphoreType.DMA((base.shape[0],)),
        ],
        compiler_params=pltpu.CompilerParams(vmem_limit_bytes=8 * 1024 * 1024),
        cost_estimate=pl.CostEstimate(
            flops=4 * 1000 * 1000 * 1000, bytes_accessed=8 * 1000 * 1000, transcendentals=0
        ),
        name="pick",
    )(kind, row, base, *tables)


def route_kernel(row_ref, shared_row_ref, own_ref, out_ref, sem):
    half = out_ref.shape[2] // 3

    def issue(chip, carry):
        shared_row = shared_row_ref[chip]
        for core in range(2):
            item = chip * 2 + core
            pltpu.make_async_copy(
                own_ref.at[row_ref[item], :, pl.ds(0, 2 * half)],
                out_ref.at[item, :, pl.ds(0, 2 * half)],
                sem,
            ).start()
            pltpu.make_async_copy(
                own_ref.at[shared_row, :, pl.ds(core * half, half)],
                out_ref.at[item, :, pl.ds(2 * half, half)],
                sem,
            ).start()
        return carry

    lax.fori_loop(0, out_ref.shape[0] // 2, issue, 0, unroll=4)
    pltpu.make_async_copy(out_ref, out_ref, sem).wait()


def route(row, shared_row, own):
    return pl.pallas_call(
        route_kernel,
        out_shape=jax.ShapeDtypeStruct(own.shape, own.dtype),
        in_specs=[pl.BlockSpec(memory_space=pltpu.SMEM)] * 2
        + [pl.BlockSpec(memory_space=pl.ANY)],
        out_specs=pl.BlockSpec(memory_space=pltpu.VMEM),
        scratch_shapes=[pltpu.SemaphoreType.DMA],
        compiler_params=pltpu.CompilerParams(vmem_limit_bytes=8 * 1024 * 1024),
        cost_estimate=pl.CostEstimate(
            flops=4 * 1000 * 1000 * 1000, bytes_accessed=12 * 1000 * 1000, transcendentals=0
        ),
        name="route",
    )(row, shared_row, own)


def place_kernel(code_ref, got_ref, other_ref, late_ref, zero_ref, out_ref, held, zeros, sems):
    rows, width = late_ref.shape
    half, step = width // 2, rows // CHUNKS
    first, second, parity = code_ref[0], code_ref[1], code_ref[2]

    def side(core):
        return pl.ds(pl.multiple_of(core * half, half), half)

    def loads(slot, code, sem):
        into = held.at[slot]

        @pl.when(code == PLAIN)
        def _():
            pltpu.make_async_copy(got_ref.at[:, pl.ds(0, width)], into, sem).start()

        @pl.when(code == LATE)
        def _():
            pltpu.make_async_copy(late_ref, into, sem).start()

        @pl.when(code == HALVES)
        def _():
            pltpu.make_async_copy(
                got_ref.at[:, pl.ds(width, half)], into.at[:, side(parity)], sem
            ).start()
            pltpu.make_async_copy(other_ref, into.at[:, side(1 - parity)], sem).start()

    for slot, code in enumerate((first, second)):
        loads(slot, code, sems.at[slot])

    pltpu.make_async_copy(zero_ref, zeros, sems.at[3]).start()
    for slot, code in enumerate((first, second)):

        @pl.when(code != EMPTY)
        def _():
            pltpu.make_async_copy(late_ref, held.at[slot], sems.at[slot]).wait()
            pltpu.make_async_copy(held.at[slot], out_ref.at[slot], sems.at[2]).start()

    pltpu.make_async_copy(zero_ref, zeros, sems.at[3]).wait()
    for slot, code in enumerate((first, second)):

        @pl.when(code == EMPTY)
        def _():
            for chunk in range(CHUNKS):
                pltpu.make_async_copy(
                    zeros, out_ref.at[slot, pl.ds(chunk * step, step), :], sems.at[2]
                ).start()

    pltpu.make_async_copy(held, out_ref, sems.at[2]).wait()


def place(codes, got, other, late):
    rows, width = late.shape
    anywhere = pl.BlockSpec(memory_space=pl.ANY)
    return pl.pallas_call(
        place_kernel,
        out_shape=jax.ShapeDtypeStruct((2, rows, width), late.dtype),
        in_specs=[pl.BlockSpec(memory_space=pltpu.SMEM)] + [anywhere] * 4,
        out_specs=anywhere,
        scratch_shapes=[
            pltpu.VMEM((2, rows, width), late.dtype),
            pltpu.VMEM((rows // CHUNKS, width), late.dtype),
            pltpu.SemaphoreType.DMA((4,)),
        ],
        compiler_params=pltpu.CompilerParams(vmem_limit_bytes=8 * 1024 * 1024),
        name="place",
    )(codes, got, other, late, jnp.zeros((rows // CHUNKS, width), late.dtype))


CHUNKS = 4


def first_kernel(index_ref, stat_ref, pending_ref, first_ref, held, sems):
    step = first_ref.shape[0] // CHUNKS
    slot = jnp.where(stat_ref[index_ref[0] * 2] >= 0, 0, 1)
    parts = [pl.ds(chunk * step, step) for chunk in range(CHUNKS)]
    loads = [
        pltpu.make_async_copy(pending_ref.at[slot, part, :], held.at[part, :], sems.at[0, pos])
        for pos, part in enumerate(parts)
    ]
    stores = [
        pltpu.make_async_copy(held.at[part, :], first_ref.at[part, :], sems.at[1, pos])
        for pos, part in enumerate(parts)
    ]
    for load in loads:
        load.start()
    for load, store in zip(loads, stores):
        load.wait()
        store.start()
    for store in stores:
        store.wait()


def first_used(my_index, pending_stat, pending_roots):
    shape, kind = pending_roots.shape[1:], pending_roots.dtype
    anywhere = pl.BlockSpec(memory_space=pl.ANY)
    return pl.pallas_call(
        first_kernel,
        out_shape=jax.ShapeDtypeStruct(shape, kind),
        in_specs=[pl.BlockSpec(memory_space=pltpu.SMEM)] * 2 + [anywhere],
        out_specs=anywhere,
        scratch_shapes=[pltpu.VMEM(shape, kind), pltpu.SemaphoreType.DMA((2, CHUNKS))],
        compiler_params=pltpu.CompilerParams(vmem_limit_bytes=8 * 1024 * 1024),
        name="first_used",
    )(my_index, pending_stat, pending_roots)


def poly_times(first, second):
    result = [0.0] * (len(first) + len(second) - 1)
    for left_pos in range(len(first)):
        for right_pos in range(len(second)):
            result[left_pos + right_pos] += first[left_pos] * second[right_pos]
    return result


def root_polynomial(iteration_count):
    x_poly = [1.0]
    m_poly = [0.0, 1.0]
    for _ in range(iteration_count):
        t_poly = [-value / 4.0 for value in m_poly]
        t_poly[0] += 5.0 / 4.0
        x_poly = poly_times(x_poly, t_poly)
        t_square = poly_times(t_poly, t_poly)
        m_poly = poly_times(poly_times(t_square, t_square), m_poly)
    return [float(value) for value in x_poly]


TILE = 256


def root_kernel(
    index_ref,
    pending_stat_ref,
    refresh_stat_ref,
    own_grad_ref,
    other_grad_ref,
    stat_ref,
    pending_ref,
    other_ref,
    new_ref,
    own_ref,
    grad_ref,
    grad,
    factor16,
    stat,
    scaled,
    scaled16,
    square,
    square16,
    cube16,
    upper16,
    root16,
    shared,
    sems,
):
    width = stat_ref.shape[0]
    half = width // 2
    tiles = width // TILE
    me = index_ref[0]
    parity = me % 2
    poly = root_polynomial(ITERS)

    def columns_of(step):
        return pl.ds(pl.multiple_of(step * TILE, TILE), TILE)

    def half_of(side):
        return pl.ds(pl.multiple_of(side * half, half), half)

    own_half = pltpu.make_async_copy(own_grad_ref, grad.at[half_of(parity), :], sems.at[0])
    other_half = pltpu.make_async_copy(other_grad_ref, grad.at[half_of(1 - parity), :], sems.at[1])
    statistic = pltpu.make_async_copy(stat_ref, stat, sems.at[2])
    grad_out = pltpu.make_async_copy(grad, grad_ref, sems.at[3])
    new_out = pltpu.make_async_copy(stat, new_ref, sems.at[4])
    second = pltpu.make_async_copy(pending_ref.at[1], root16, sems.at[5])
    shared_in = pltpu.make_async_copy(other_ref, shared, sems.at[6])
    shared_out = pltpu.make_async_copy(shared, own_ref.at[:, pl.ds(width, half)], sems.at[7])

    def root_out(step):
        return pltpu.make_async_copy(
            root16.at[:, columns_of(step)], own_ref.at[:, columns_of(step)], sems.at[8]
        )

    own_half.start()
    other_half.start()
    statistic.start()

    def look(item, found):
        entry = refresh_stat_ref[item]
        return found[0] | (entry == me), found[1] | (entry == me - parity)

    refreshed, core_refreshed = lax.fori_loop(
        0, refresh_stat_ref.shape[0], look, (jnp.bool_(False), jnp.bool_(False)), unroll=16
    )
    core = (me - parity) * 2
    core_shares = (
        core_refreshed & (pending_stat_ref[core] >= 0) & (pending_stat_ref[core + 1] >= 0)
    )
    from_other = core_shares == (parity == 1)

    @pl.when(from_other)
    def _():
        shared_in.start()

    @pl.when(jnp.logical_not(from_other))
    def _():
        pltpu.make_async_copy(
            pending_ref.at[1, :, half_of(parity)], shared, sems.at[6]
        ).start()

    @pl.when(jnp.logical_not(refreshed))
    def _():
        second.start()

    own_half.wait()
    other_half.wait()
    grad_out.start()

    @pl.when(parity == 0)
    def _():
        factor16[...] = grad[...]

    @pl.when(parity == 1)
    def _():
        @pl.loop(0, tiles)
        def _(step):
            columns = columns_of(step)
            factor16[columns, :] = jnp.transpose(grad[:, columns])

    statistic.wait()

    def update(step, trace):
        columns = columns_of(step)
        gram = lax.dot_general(
            factor16[...],
            factor16[columns, :],
            (((1,), (1,)), ((), ())),
            preferred_element_type=jnp.float32,
        )
        stat[:, columns] = decay_rate * stat[:, columns] + (1.0 - decay_rate) * gram
        block = stat[columns, columns]
        on_diagonal = lax.broadcasted_iota(jnp.int32, (TILE, TILE), 0) == lax.broadcasted_iota(
            jnp.int32, (TILE, TILE), 1
        )
        return trace + jnp.sum(jnp.where(on_diagonal, block, 0.0), axis=0, keepdims=True)

    diagonal = lax.fori_loop(0, tiles, update, jnp.zeros((1, TILE), jnp.float32))
    shared_in.wait()
    shared_out.start()

    @pl.when(jnp.logical_not(refreshed))
    def _():
        second.wait()
        new_out.start()
        for step in range(tiles):
            root_out(step).start()

    @pl.when(refreshed)
    def _():
        norm_scale = 2.0 * jnp.sum(diagonal, axis=1, keepdims=True) / width
        factor = lax.rsqrt(jnp.sqrt(norm_scale))

        @pl.loop(0, width // 128)
        def _(step):
            rows = pl.ds(pl.multiple_of(step * 128, 128), 128)
            part = stat[rows, :] / norm_scale
            scaled[rows, :] = part
            scaled16[rows, :] = part.astype(jnp.bfloat16)

        new_out.start()

        def identity(step):
            return (
                lax.broadcasted_iota(jnp.int32, (width, TILE), 0)
                == lax.broadcasted_iota(jnp.int32, (width, TILE), 1) + step * TILE
            )

        def dot(first, second):
            return jnp.dot(first, second, preferred_element_type=jnp.float32)

        @pl.loop(0, tiles)
        def _(step):
            columns = columns_of(step)
            tile = dot(scaled16[...], scaled16[:, columns])
            square[:, columns] = tile
            square16[:, columns] = tile.astype(jnp.bfloat16)

        @pl.loop(0, tiles)
        def _(step):
            columns = columns_of(step)
            cube = dot(square16[...], scaled16[:, columns])
            cube16[:, columns] = cube.astype(jnp.bfloat16)
            upper = (
                jnp.where(identity(step), poly[3], 0.0)
                + poly[4] * scaled[:, columns]
                + poly[5] * square[:, columns]
                + poly[6] * cube
            )
            upper16[:, columns] = upper.astype(jnp.bfloat16)

        @pl.loop(0, tiles)
        def _(step):
            columns = columns_of(step)
            total = dot(cube16[...], upper16[:, columns])
            total += (
                jnp.where(identity(step), poly[0], 0.0)
                + poly[1] * scaled[:, columns]
                + poly[2] * square[:, columns]
            )
            root16[:, columns] = (total * factor).astype(jnp.bfloat16)

            @pl.when(step > 0)
            def _():
                root_out(step - 1).start()

    grad_out.wait()
    new_out.wait()

    @pl.when(refreshed)
    def _():
        root_out(tiles - 1).start()

    shared_out.wait()
    pltpu.make_async_copy(root16, own_ref.at[:, pl.ds(0, width)], sems.at[8]).wait()


def updated_and_root(
    my_index, pending_stat, refresh_stat, own_grad, other_grad, statistic, pending_roots, columns
):
    width = statistic.shape[0]
    anywhere = pl.BlockSpec(memory_space=pl.ANY)
    plain = pltpu.VMEM((width, width), jnp.float32)
    short = pltpu.VMEM((width, width), jnp.bfloat16)
    return pl.pallas_call(
        root_kernel,
        out_shape=(
            jax.ShapeDtypeStruct((width, width), jnp.float32),
            jax.ShapeDtypeStruct((width, width + width // 2), jnp.bfloat16),
            jax.ShapeDtypeStruct((width, width), jnp.bfloat16),
        ),
        in_specs=[pl.BlockSpec(memory_space=pltpu.SMEM)] * 3 + [anywhere] * 5,
        out_specs=(anywhere,) * 3,
        scratch_shapes=[
            short,
            short,
            plain,
            plain,
            short,
            plain,
            short,
            short,
            short,
            short,
            pltpu.VMEM((width, width // 2), jnp.bfloat16),
            pltpu.SemaphoreType.DMA((9,)),
        ],
        compiler_params=pltpu.CompilerParams(vmem_limit_bytes=44 * 1024 * 1024),
        cost_estimate=pl.CostEstimate(
            flops=8 * width**3, bytes_accessed=17 * width * width, transcendentals=0
        ),
        name="root",
    )(
        my_index,
        pending_stat,
        refresh_stat,
        own_grad,
        other_grad,
        statistic,
        pending_roots,
        columns,
    )


def per_device(gradient, statistics, held_roots, pending_roots, pending_stat, refresh_stat):
    devices = lax.axis_size("dev")
    my_index = lax.axis_index("dev")
    parity = my_index % 2
    block_width = statistics.shape[1]
    piece_rows = block_width // devices
    slot_count = pending_roots.shape[0]
    half_rows = gradient.shape[0]
    half_columns = block_width // 2
    slot_total = pending_stat.shape[0]
    device_ids = jnp.arange(devices, dtype=jnp.int32)

    index_table = my_index.reshape(1)
    first_root = first_used(index_table, pending_stat, pending_roots)
    first_parts = spread(first_root.reshape(devices, piece_rows, block_width))
    cut_columns = lax.dynamic_slice(
        pending_roots, (1, 0, (1 - parity) * half_columns), (1, block_width, half_columns)
    )[0]
    other_columns = swapped(cut_columns, "dev", 0)

    new_stat, own_matrix, full_grad = updated_and_root(
        index_table,
        pending_stat,
        refresh_stat,
        gradient,
        swapped(gradient, "dev", 0),
        statistics[0],
        pending_roots,
        other_columns,
    )
    root_parts = spread(own_matrix.reshape(devices, piece_rows, block_width + half_columns))

    has_first = pending_stat.reshape(devices, slot_count)[:, 0] >= 0
    has_second = has_first & (pending_stat.reshape(devices, slot_count)[:, 1] >= 0)
    refreshed = jnp.any(refresh_stat[None, :] == device_ids[:, None], axis=1)
    sharing_pairs = (has_second & refreshed).reshape(devices // 2, 2)
    unplaced = jnp.any(sharing_pairs[:, 0] & sharing_pairs[:, 1])
    slot_ids = jnp.arange(slot_total, dtype=jnp.int32)
    slot_match = pending_stat[None, :] == device_ids[:, None]
    found = jnp.any(slot_match, axis=1)
    slot_of = jnp.sum(jnp.where(slot_match, slot_ids[None, :], 0), axis=1)
    is_second = jnp.any(
        slot_match & (slot_ids % slot_count == 1) & jnp.repeat(has_first, slot_count), axis=1
    )
    is_shared = jnp.any(slot_match & jnp.repeat(refreshed, slot_count), axis=1)
    is_extra = jnp.any(
        slot_match
        & (slot_ids // slot_count % 2 == 1)
        & jnp.repeat(sharing_pairs[:, 0], 2 * slot_count),
        axis=1,
    )
    shared_kind = jnp.where(is_extra, EXTRA, SHARED)
    kind = jnp.where(is_second, jnp.where(is_shared, shared_kind, OWN), FIRST)

    wanted = refresh_stat.reshape(devices, slot_count)
    wants_two = (wanted[:, 0] >= 0) & (wanted[:, 1] >= 0)
    two_pairs = wants_two.reshape(devices // 2, 2)
    second_pairs = jnp.maximum(wanted[:, 1], 0).reshape(devices // 2, 2)
    first_wanted = jnp.maximum(jnp.where(wanted[:, 0] >= 0, wanted[:, 0], wanted[:, 1]), 0)
    shared_wanted = jnp.where(two_pairs[:, 0], second_pairs[:, 0], second_pairs[:, 1])
    fourth = two_pairs[:, 0] & two_pairs[:, 1]
    found_pairs = found.reshape(devices // 2, 2)
    unrouted = jnp.any(fourth & found_pairs[:, 0] & found_pairs[:, 1])
    carries = (
        jnp.repeat(fourth, 2)
        & jnp.logical_not(found)
        & ((device_ids % 2 == 1) | jnp.repeat(found_pairs[:, 1], 2))
    )
    kind = jnp.where(carries, OWN, kind).astype(jnp.int32)
    source = jnp.where(carries, jnp.repeat(second_pairs[:, 1], 2), slot_of // slot_count)

    base = gather(slot_of // slot_count, first_parts)

    def choose(more_pending, more_fresh):
        def run():
            tables = [base, root_parts]
            if more_pending:
                columns = jnp.where(
                    parity == 0, other_columns, pending_roots[1][:, half_columns:]
                )
                tables.append(spread(columns.reshape(devices, piece_rows, half_columns)))
            chosen, spare = pick(kind, source, *tables)
            if more_fresh:
                late, _ = pick(
                    jnp.full((devices,), OWN, jnp.int32), jnp.maximum(wanted[:, 1], 0), *tables[:2]
                )
                spare = spread(late)
            return chosen, spare

        return run

    chosen, spare = lax.switch(
        unplaced + 2 * unrouted.astype(jnp.int32),
        [choose(more % 2 == 1, more // 2 == 1) for more in range(4)],
    )
    chosen, spare = lax.optimization_barrier((chosen, spare))
    returned = spread(chosen).reshape(block_width, block_width)
    routed = route(first_wanted, shared_wanted, root_parts)
    fresh = spread(routed).reshape(block_width, block_width + half_columns)

    my_found = jnp.any(pending_stat == my_index)
    partner_found = jnp.any(pending_stat == my_index + 1 - 2 * parity)
    other_returned = swapped(jnp.where(my_found, held_roots[0], returned), "dev", 0)
    merged = lax.optimization_barrier(jnp.where(my_found, returned, held_roots[0]))
    late = jnp.where(
        my_found,
        jnp.where(partner_found, spare.reshape(block_width, block_width), other_returned),
        returned,
    )

    partner_root = swapped(merged, "dev", 0)
    left_root = jnp.where(parity == 0, merged, partner_root)
    right_root = jnp.where(parity == 0, partner_root, merged)
    left_rows = lax.dynamic_slice_in_dim(left_root, parity * half_rows, half_rows, 0)
    left_times = jnp.dot(left_rows, full_grad, preferred_element_type=jnp.float32).astype(
        jnp.bfloat16
    )
    product = jnp.dot(left_times, right_root, preferred_element_type=jnp.float32)
    own_square = jnp.sum(product * product)
    other_square = swapped(own_square, "dev", 0)
    rms_scale = lax.rsqrt((own_square + other_square) / (block_width * block_width) + 1e-06)
    direction = (product * rms_scale).astype(jnp.bfloat16)

    my_slots = lax.dynamic_slice_in_dim(refresh_stat, my_index * slot_count, slot_count, 0)
    core_slots = lax.dynamic_slice_in_dim(
        refresh_stat, (my_index - parity) * slot_count, slot_count, 0
    )
    is_fourth = (parity == 1) & jnp.all(core_slots >= 0)
    doubled = jnp.where(is_fourth, LATE, HALVES)
    codes = jnp.stack(
        [
            jnp.where(my_slots[0] >= 0, PLAIN, EMPTY),
            jnp.where(my_slots[1] >= 0, jnp.where(my_slots[0] >= 0, doubled, PLAIN), EMPTY),
            parity,
        ]
    ).astype(jnp.int32)
    fresh, direction, codes, late = lax.optimization_barrier((fresh, direction, codes, late))
    fresh_roots = place(codes, fresh, swapped(fresh[:, block_width:], "dev", 0), late)
    return (new_stat[None], merged[None], direction, fresh_roots)


def solution(mesh):
    in_specs = (
        P("dev", None),
        P("dev", None, None),
        P("dev", None, None),
        P("dev", None, None),
        P(),
        P(),
    )
    out_specs = (P("dev", None, None), P("dev", None, None), P("dev", None), P("dev", None, None))
    return jax.shard_map(
        per_device, mesh=mesh, in_specs=in_specs, out_specs=out_specs, check_vma=False
    )
```

```python
import jax
import jax.numpy as jnp
from jax import lax
from jax.experimental import pallas as pl
from jax.experimental.pallas import tpu as pltpu
from jax.sharding import PartitionSpec as P


ITERS = 2


decay_rate = 0.9


def swapped(shard, axis, bit):
    return lax.ppermute(shard, axis, [(i, i ^ 1 << bit) for i in range(lax.axis_size(axis))])


def spread(parts):
    return lax.all_to_all(parts, "dev", split_axis=0, concat_axis=0, tiled=True)


CHUNKS = 4
FIRST, OWN, SHARED, EXTRA = range(4)
EMPTY, PLAIN, HALVES, LATE = range(4)


def pick_kernel(kind_ref, row_ref, own_ref, *refs):
    tables, result_ref, out_ref, sems = refs[:-4], refs[-4], refs[-2], refs[-1]
    width = out_ref.shape[2]
    half, span = width // 2, out_ref.shape[0] // CHUNKS

    def issue(item, carry):
        row, kind = row_ref[item], kind_ref[item]

        def start(src, dst):
            pltpu.make_async_copy(src, dst, sems.at[0, item // span]).start()

        @pl.when(kind == FIRST)
        def _():
            start(tables[0].at[row], out_ref.at[item])

        @pl.when(kind != FIRST)
        def _():
            @pl.when(kind == OWN)
            def _():
                start(own_ref.at[row, :, pl.ds(0, width)], out_ref.at[item])

            @pl.when(kind == SHARED)
            def _():
                for core in range(2):
                    start(
                        own_ref.at[row // 2 * 2 + core, :, pl.ds(width, half)],
                        out_ref.at[item, :, pl.ds(core * half, half)],
                    )

            if len(tables) > 1:

                @pl.when(kind == EXTRA)
                def _():
                    for core in range(2):
                        start(
                            tables[1].at[row // 2 * 2 + core],
                            out_ref.at[item, :, pl.ds(core * half, half)],
                        )

        return carry

    parts = [pl.ds(chunk * span, span) for chunk in range(CHUNKS)]
    stores = [
        pltpu.make_async_copy(out_ref.at[part], result_ref.at[part], sems.at[1, chunk])
        for chunk, part in enumerate(parts)
    ]

    def pass_on(chunk):
        part = out_ref.at[parts[chunk]]
        pltpu.make_async_copy(part, part, sems.at[0, chunk]).wait()
        stores[chunk].start()

    for chunk in range(CHUNKS):
        lax.fori_loop(chunk * span, (chunk + 1) * span, issue, 0, unroll=8)
        if chunk:
            pass_on(chunk - 1)
    pass_on(CHUNKS - 1)
    for store in stores:
        store.wait()


def pick(kind, row, *tables):
    items, (_, piece_rows, width) = row.shape[0], tables[1].shape
    shape = jax.ShapeDtypeStruct((items, piece_rows, width), tables[0].dtype)
    anywhere = pl.BlockSpec(memory_space=pl.ANY)
    return pl.pallas_call(
        pick_kernel,
        out_shape=(shape, shape),
        in_specs=[pl.BlockSpec(memory_space=pltpu.SMEM)] * 2 + [anywhere] * len(tables),
        out_specs=(anywhere, anywhere),
        scratch_shapes=[
            pltpu.VMEM(shape.shape, shape.dtype),
            pltpu.SemaphoreType.DMA((2, CHUNKS)),
        ],
        compiler_params=pltpu.CompilerParams(vmem_limit_bytes=8 * 1024 * 1024),
        cost_estimate=pl.CostEstimate(
            flops=4 * 1000 * 1000 * 1000, bytes_accessed=8 * 1000 * 1000, transcendentals=0
        ),
        name="pick",
    )(kind, row, *tables)


def route_kernel(row_ref, shared_row_ref, own_ref, out_ref, sem):
    half = out_ref.shape[2] // 3

    def issue(chip, carry):
        shared_row = shared_row_ref[chip]
        for core in range(2):
            item = chip * 2 + core
            pltpu.make_async_copy(
                own_ref.at[row_ref[item], :, pl.ds(0, 2 * half)],
                out_ref.at[item, :, pl.ds(0, 2 * half)],
                sem,
            ).start()
            pltpu.make_async_copy(
                own_ref.at[shared_row, :, pl.ds(core * half, half)],
                out_ref.at[item, :, pl.ds(2 * half, half)],
                sem,
            ).start()
        return carry

    lax.fori_loop(0, out_ref.shape[0] // 2, issue, 0, unroll=4)
    pltpu.make_async_copy(out_ref, out_ref, sem).wait()


def route(row, shared_row, own):
    return pl.pallas_call(
        route_kernel,
        out_shape=jax.ShapeDtypeStruct(own.shape, own.dtype),
        in_specs=[pl.BlockSpec(memory_space=pltpu.SMEM)] * 2
        + [pl.BlockSpec(memory_space=pl.ANY)],
        out_specs=pl.BlockSpec(memory_space=pltpu.VMEM),
        scratch_shapes=[pltpu.SemaphoreType.DMA],
        compiler_params=pltpu.CompilerParams(vmem_limit_bytes=8 * 1024 * 1024),
        cost_estimate=pl.CostEstimate(
            flops=4 * 1000 * 1000 * 1000, bytes_accessed=12 * 1000 * 1000, transcendentals=0
        ),
        name="route",
    )(row, shared_row, own)


def place_kernel(code_ref, got_ref, other_ref, late_ref, zero_ref, out_ref, held, zeros, sems):
    rows, width = late_ref.shape
    half, step = width // 2, rows // CHUNKS
    first, second, parity = code_ref[0], code_ref[1], code_ref[2]

    def side(core):
        return pl.ds(pl.multiple_of(core * half, half), half)

    def loads(slot, code, sem):
        into = held.at[slot]

        @pl.when(code == PLAIN)
        def _():
            pltpu.make_async_copy(got_ref.at[:, pl.ds(0, width)], into, sem).start()

        @pl.when(code == LATE)
        def _():
            pltpu.make_async_copy(late_ref, into, sem).start()

        @pl.when(code == HALVES)
        def _():
            pltpu.make_async_copy(
                got_ref.at[:, pl.ds(width, half)], into.at[:, side(parity)], sem
            ).start()
            pltpu.make_async_copy(other_ref, into.at[:, side(1 - parity)], sem).start()

    for slot, code in enumerate((first, second)):
        loads(slot, code, sems.at[slot])

    pltpu.make_async_copy(zero_ref, zeros, sems.at[3]).start()
    for slot, code in enumerate((first, second)):

        @pl.when(code != EMPTY)
        def _():
            pltpu.make_async_copy(late_ref, held.at[slot], sems.at[slot]).wait()
            pltpu.make_async_copy(held.at[slot], out_ref.at[slot], sems.at[2]).start()

    pltpu.make_async_copy(zero_ref, zeros, sems.at[3]).wait()
    for slot, code in enumerate((first, second)):

        @pl.when(code == EMPTY)
        def _():
            for chunk in range(CHUNKS):
                pltpu.make_async_copy(
                    zeros, out_ref.at[slot, pl.ds(chunk * step, step), :], sems.at[2]
                ).start()

    pltpu.make_async_copy(held, out_ref, sems.at[2]).wait()


def place(codes, got, other, late):
    rows, width = late.shape
    anywhere = pl.BlockSpec(memory_space=pl.ANY)
    return pl.pallas_call(
        place_kernel,
        out_shape=jax.ShapeDtypeStruct((2, rows, width), late.dtype),
        in_specs=[pl.BlockSpec(memory_space=pltpu.SMEM)] + [anywhere] * 4,
        out_specs=anywhere,
        scratch_shapes=[
            pltpu.VMEM((2, rows, width), late.dtype),
            pltpu.VMEM((rows // CHUNKS, width), late.dtype),
            pltpu.SemaphoreType.DMA((4,)),
        ],
        compiler_params=pltpu.CompilerParams(vmem_limit_bytes=8 * 1024 * 1024),
        name="place",
    )(codes, got, other, late, jnp.zeros((rows // CHUNKS, width), late.dtype))


def first_kernel(index_ref, stat_ref, pending_ref, first_ref, held, sems):
    step = first_ref.shape[0] // CHUNKS
    slot = jnp.where(stat_ref[index_ref[0] * 2] >= 0, 0, 1)
    parts = [pl.ds(chunk * step, step) for chunk in range(CHUNKS)]
    loads = [
        pltpu.make_async_copy(pending_ref.at[slot, part, :], held.at[part, :], sems.at[0, pos])
        for pos, part in enumerate(parts)
    ]
    stores = [
        pltpu.make_async_copy(held.at[part, :], first_ref.at[part, :], sems.at[1, pos])
        for pos, part in enumerate(parts)
    ]
    for load in loads:
        load.start()
    for load, store in zip(loads, stores):
        load.wait()
        store.start()
    for store in stores:
        store.wait()


def first_used(my_index, pending_stat, pending_roots):
    shape, kind = pending_roots.shape[1:], pending_roots.dtype
    anywhere = pl.BlockSpec(memory_space=pl.ANY)
    return pl.pallas_call(
        first_kernel,
        out_shape=jax.ShapeDtypeStruct(shape, kind),
        in_specs=[pl.BlockSpec(memory_space=pltpu.SMEM)] * 2 + [anywhere],
        out_specs=anywhere,
        scratch_shapes=[pltpu.VMEM(shape, kind), pltpu.SemaphoreType.DMA((2, CHUNKS))],
        compiler_params=pltpu.CompilerParams(vmem_limit_bytes=8 * 1024 * 1024),
        name="first_used",
    )(my_index, pending_stat, pending_roots)


def poly_times(first, second):
    result = [0.0] * (len(first) + len(second) - 1)
    for left_pos in range(len(first)):
        for right_pos in range(len(second)):
            result[left_pos + right_pos] += first[left_pos] * second[right_pos]
    return result


def root_polynomial(iteration_count):
    x_poly = [1.0]
    m_poly = [0.0, 1.0]
    for _ in range(iteration_count):
        t_poly = [-value / 4.0 for value in m_poly]
        t_poly[0] += 5.0 / 4.0
        x_poly = poly_times(x_poly, t_poly)
        t_square = poly_times(t_poly, t_poly)
        m_poly = poly_times(poly_times(t_square, t_square), m_poly)
    return [float(value) for value in x_poly]


TILE = 256


def root_kernel(
    index_ref,
    pending_stat_ref,
    refresh_stat_ref,
    own_grad_ref,
    other_grad_ref,
    stat_ref,
    pending_ref,
    other_ref,
    new_ref,
    own_ref,
    grad_ref,
    grad,
    factor16,
    stat,
    scaled,
    scaled16,
    square,
    square16,
    cube16,
    upper16,
    root16,
    shared,
    sems,
):
    width = stat_ref.shape[0]
    half = width // 2
    tiles = width // TILE
    me = index_ref[0]
    parity = me % 2
    poly = root_polynomial(ITERS)

    def columns_of(step):
        return pl.ds(pl.multiple_of(step * TILE, TILE), TILE)

    def half_of(side):
        return pl.ds(pl.multiple_of(side * half, half), half)

    own_half = pltpu.make_async_copy(own_grad_ref, grad.at[half_of(parity), :], sems.at[0])
    other_half = pltpu.make_async_copy(other_grad_ref, grad.at[half_of(1 - parity), :], sems.at[1])
    statistic = pltpu.make_async_copy(stat_ref, stat, sems.at[2])
    grad_out = pltpu.make_async_copy(grad, grad_ref, sems.at[3])
    new_out = pltpu.make_async_copy(stat, new_ref, sems.at[4])
    second = pltpu.make_async_copy(pending_ref.at[1], root16, sems.at[5])
    shared_in = pltpu.make_async_copy(other_ref, shared, sems.at[6])
    shared_out = pltpu.make_async_copy(shared, own_ref.at[:, pl.ds(width, half)], sems.at[7])

    def root_out(step):
        return pltpu.make_async_copy(
            root16.at[:, columns_of(step)], own_ref.at[:, columns_of(step)], sems.at[8]
        )

    own_half.start()
    other_half.start()
    statistic.start()

    def look(item, found):
        entry = refresh_stat_ref[item]
        return found[0] | (entry == me), found[1] | (entry == me - parity)

    refreshed, core_refreshed = lax.fori_loop(
        0, refresh_stat_ref.shape[0], look, (jnp.bool_(False), jnp.bool_(False)), unroll=16
    )
    core = (me - parity) * 2
    core_shares = (
        core_refreshed & (pending_stat_ref[core] >= 0) & (pending_stat_ref[core + 1] >= 0)
    )
    from_other = core_shares == (parity == 1)

    @pl.when(from_other)
    def _():
        shared_in.start()

    @pl.when(jnp.logical_not(from_other))
    def _():
        pltpu.make_async_copy(
            pending_ref.at[1, :, half_of(parity)], shared, sems.at[6]
        ).start()

    @pl.when(jnp.logical_not(refreshed))
    def _():
        second.start()

    own_half.wait()
    other_half.wait()
    grad_out.start()

    @pl.when(parity == 0)
    def _():
        factor16[...] = grad[...]

    @pl.when(parity == 1)
    def _():
        @pl.loop(0, tiles)
        def _(step):
            columns = columns_of(step)
            factor16[columns, :] = jnp.transpose(grad[:, columns])

    statistic.wait()

    def update(step, trace):
        columns = columns_of(step)
        gram = lax.dot_general(
            factor16[...],
            factor16[columns, :],
            (((1,), (1,)), ((), ())),
            preferred_element_type=jnp.float32,
        )
        stat[:, columns] = decay_rate * stat[:, columns] + (1.0 - decay_rate) * gram
        block = stat[columns, columns]
        on_diagonal = lax.broadcasted_iota(jnp.int32, (TILE, TILE), 0) == lax.broadcasted_iota(
            jnp.int32, (TILE, TILE), 1
        )
        return trace + jnp.sum(jnp.where(on_diagonal, block, 0.0), axis=0, keepdims=True)

    diagonal = lax.fori_loop(0, tiles, update, jnp.zeros((1, TILE), jnp.float32))
    shared_in.wait()
    shared_out.start()

    @pl.when(jnp.logical_not(refreshed))
    def _():
        second.wait()
        new_out.start()
        for step in range(tiles):
            root_out(step).start()

    @pl.when(refreshed)
    def _():
        norm_scale = 2.0 * jnp.sum(diagonal, axis=1, keepdims=True) / width
        factor = lax.rsqrt(jnp.sqrt(norm_scale))

        @pl.loop(0, width // 128)
        def _(step):
            rows = pl.ds(pl.multiple_of(step * 128, 128), 128)
            part = stat[rows, :] / norm_scale
            scaled[rows, :] = part
            scaled16[rows, :] = part.astype(jnp.bfloat16)

        new_out.start()

        def identity(step):
            return (
                lax.broadcasted_iota(jnp.int32, (width, TILE), 0)
                == lax.broadcasted_iota(jnp.int32, (width, TILE), 1) + step * TILE
            )

        def dot(first, second):
            return jnp.dot(first, second, preferred_element_type=jnp.float32)

        @pl.loop(0, tiles)
        def _(step):
            columns = columns_of(step)
            tile = dot(scaled16[...], scaled16[:, columns])
            square[:, columns] = tile
            square16[:, columns] = tile.astype(jnp.bfloat16)

        @pl.loop(0, tiles)
        def _(step):
            columns = columns_of(step)
            cube = dot(square16[...], scaled16[:, columns])
            cube16[:, columns] = cube.astype(jnp.bfloat16)
            upper = (
                jnp.where(identity(step), poly[3], 0.0)
                + poly[4] * scaled[:, columns]
                + poly[5] * square[:, columns]
                + poly[6] * cube
            )
            upper16[:, columns] = upper.astype(jnp.bfloat16)

        @pl.loop(0, tiles)
        def _(step):
            columns = columns_of(step)
            total = dot(cube16[...], upper16[:, columns])
            total += (
                jnp.where(identity(step), poly[0], 0.0)
                + poly[1] * scaled[:, columns]
                + poly[2] * square[:, columns]
            )
            root16[:, columns] = (total * factor).astype(jnp.bfloat16)

            @pl.when(step > 0)
            def _():
                root_out(step - 1).start()

    grad_out.wait()
    new_out.wait()

    @pl.when(refreshed)
    def _():
        root_out(tiles - 1).start()

    shared_out.wait()
    pltpu.make_async_copy(root16, own_ref.at[:, pl.ds(0, width)], sems.at[8]).wait()


def updated_and_root(
    my_index, pending_stat, refresh_stat, own_grad, other_grad, statistic, pending_roots, columns
):
    width = statistic.shape[0]
    anywhere = pl.BlockSpec(memory_space=pl.ANY)
    plain = pltpu.VMEM((width, width), jnp.float32)
    short = pltpu.VMEM((width, width), jnp.bfloat16)
    return pl.pallas_call(
        root_kernel,
        out_shape=(
            jax.ShapeDtypeStruct((width, width), jnp.float32),
            jax.ShapeDtypeStruct((width, width + width // 2), jnp.bfloat16),
            jax.ShapeDtypeStruct((width, width), jnp.bfloat16),
        ),
        in_specs=[pl.BlockSpec(memory_space=pltpu.SMEM)] * 3 + [anywhere] * 5,
        out_specs=(anywhere,) * 3,
        scratch_shapes=[
            short,
            short,
            plain,
            plain,
            short,
            plain,
            short,
            short,
            short,
            short,
            pltpu.VMEM((width, width // 2), jnp.bfloat16),
            pltpu.SemaphoreType.DMA((9,)),
        ],
        compiler_params=pltpu.CompilerParams(vmem_limit_bytes=44 * 1024 * 1024),
        cost_estimate=pl.CostEstimate(
            flops=8 * width**3, bytes_accessed=17 * width * width, transcendentals=0
        ),
        name="root",
    )(
        my_index,
        pending_stat,
        refresh_stat,
        own_grad,
        other_grad,
        statistic,
        pending_roots,
        columns,
    )


def per_device(gradient, statistics, held_roots, pending_roots, pending_stat, refresh_stat):
    devices = lax.axis_size("dev")
    my_index = lax.axis_index("dev")
    parity = my_index % 2
    block_width = statistics.shape[1]
    piece_rows = block_width // devices
    slot_count = pending_roots.shape[0]
    half_rows = gradient.shape[0]
    half_columns = block_width // 2
    slot_total = pending_stat.shape[0]
    device_ids = jnp.arange(devices, dtype=jnp.int32)

    index_table = my_index.reshape(1)
    first_root = first_used(index_table, pending_stat, pending_roots)
    first_parts = spread(first_root.reshape(devices, piece_rows, block_width))
    cut_columns = lax.dynamic_slice(
        pending_roots, (1, 0, (1 - parity) * half_columns), (1, block_width, half_columns)
    )[0]
    other_columns = swapped(cut_columns, "dev", 0)

    new_stat, own_matrix, full_grad = updated_and_root(
        index_table,
        pending_stat,
        refresh_stat,
        gradient,
        swapped(gradient, "dev", 0),
        statistics[0],
        pending_roots,
        other_columns,
    )
    root_parts = spread(own_matrix.reshape(devices, piece_rows, block_width + half_columns))

    has_first = pending_stat.reshape(devices, slot_count)[:, 0] >= 0
    has_second = has_first & (pending_stat.reshape(devices, slot_count)[:, 1] >= 0)
    refreshed = jnp.any(refresh_stat[None, :] == device_ids[:, None], axis=1)
    sharing_pairs = (has_second & refreshed).reshape(devices // 2, 2)
    unplaced = jnp.any(sharing_pairs[:, 0] & sharing_pairs[:, 1])
    slot_ids = jnp.arange(slot_total, dtype=jnp.int32)
    slot_match = pending_stat[None, :] == device_ids[:, None]
    found = jnp.any(slot_match, axis=1)
    slot_of = jnp.sum(jnp.where(slot_match, slot_ids[None, :], 0), axis=1)
    is_second = jnp.any(
        slot_match & (slot_ids % slot_count == 1) & jnp.repeat(has_first, slot_count), axis=1
    )
    is_shared = jnp.any(slot_match & jnp.repeat(refreshed, slot_count), axis=1)
    is_extra = jnp.any(
        slot_match
        & (slot_ids // slot_count % 2 == 1)
        & jnp.repeat(sharing_pairs[:, 0], 2 * slot_count),
        axis=1,
    )
    shared_kind = jnp.where(is_extra, EXTRA, SHARED)
    kind = jnp.where(is_second, jnp.where(is_shared, shared_kind, OWN), FIRST)

    wanted = refresh_stat.reshape(devices, slot_count)
    wants_two = (wanted[:, 0] >= 0) & (wanted[:, 1] >= 0)
    two_pairs = wants_two.reshape(devices // 2, 2)
    second_pairs = jnp.maximum(wanted[:, 1], 0).reshape(devices // 2, 2)
    first_wanted = jnp.maximum(jnp.where(wanted[:, 0] >= 0, wanted[:, 0], wanted[:, 1]), 0)
    shared_wanted = jnp.where(two_pairs[:, 0], second_pairs[:, 0], second_pairs[:, 1])
    fourth = two_pairs[:, 0] & two_pairs[:, 1]
    found_pairs = found.reshape(devices // 2, 2)
    unrouted = jnp.any(fourth & found_pairs[:, 0] & found_pairs[:, 1])
    carries = (
        jnp.repeat(fourth, 2)
        & jnp.logical_not(found)
        & ((device_ids % 2 == 1) | jnp.repeat(found_pairs[:, 1], 2))
    )
    kind = jnp.where(carries, OWN, kind).astype(jnp.int32)
    source = jnp.where(carries, jnp.repeat(second_pairs[:, 1], 2), slot_of // slot_count)

    def choose(more_pending, more_fresh):
        def run():
            tables = [root_parts, first_parts]
            if more_pending:
                columns = jnp.where(
                    parity == 0, other_columns, pending_roots[1][:, half_columns:]
                )
                tables.append(spread(columns.reshape(devices, piece_rows, half_columns)))
            chosen, spare = pick(kind, source, *tables)
            if more_fresh:
                late, _ = pick(
                    jnp.full((devices,), OWN, jnp.int32), jnp.maximum(wanted[:, 1], 0), *tables[:2]
                )
                spare = spread(late)
            return chosen, spare

        return run

    chosen, spare = lax.switch(
        unplaced + 2 * unrouted.astype(jnp.int32),
        [choose(more % 2 == 1, more // 2 == 1) for more in range(4)],
    )
    chosen, spare = lax.optimization_barrier((chosen, spare))
    returned = spread(chosen).reshape(block_width, block_width)
    routed = route(first_wanted, shared_wanted, root_parts)
    fresh = spread(routed).reshape(block_width, block_width + half_columns)

    my_found = jnp.any(pending_stat == my_index)
    partner_found = jnp.any(pending_stat == my_index + 1 - 2 * parity)
    other_returned = swapped(returned, "dev", 0)
    merged = lax.optimization_barrier(jnp.where(my_found, returned, held_roots[0]))
    late = jnp.where(
        my_found,
        jnp.where(partner_found, spare.reshape(block_width, block_width), other_returned),
        returned,
    )

    partner_root = swapped(merged, "dev", 0)
    left_root = jnp.where(parity == 0, merged, partner_root)
    right_root = jnp.where(parity == 0, partner_root, merged)
    left_rows = lax.dynamic_slice_in_dim(left_root, parity * half_rows, half_rows, 0)
    left_times = jnp.dot(left_rows, full_grad, preferred_element_type=jnp.float32).astype(
        jnp.bfloat16
    )
    product = jnp.dot(left_times, right_root, preferred_element_type=jnp.float32)
    own_square = jnp.sum(product * product)
    other_square = swapped(own_square, "dev", 0)
    rms_scale = lax.rsqrt((own_square + other_square) / (block_width * block_width) + 1e-06)
    direction = (product * rms_scale).astype(jnp.bfloat16)

    my_slots = lax.dynamic_slice_in_dim(refresh_stat, my_index * slot_count, slot_count, 0)
    core_slots = lax.dynamic_slice_in_dim(
        refresh_stat, (my_index - parity) * slot_count, slot_count, 0
    )
    is_fourth = (parity == 1) & jnp.all(core_slots >= 0)
    doubled = jnp.where(is_fourth, LATE, HALVES)
    codes = jnp.stack(
        [
            jnp.where(my_slots[0] >= 0, PLAIN, EMPTY),
            jnp.where(my_slots[1] >= 0, jnp.where(my_slots[0] >= 0, doubled, PLAIN), EMPTY),
            parity,
        ]
    ).astype(jnp.int32)
    fresh, direction, codes, late = lax.optimization_barrier((fresh, direction, codes, late))
    fresh_roots = place(codes, fresh, swapped(fresh[:, block_width:], "dev", 0), late)
    return (new_stat[None], merged[None], direction, fresh_roots)


def solution(mesh):
    in_specs = (
        P("dev", None),
        P("dev", None, None),
        P("dev", None, None),
        P("dev", None, None),
        P(),
        P(),
    )
    out_specs = (P("dev", None, None), P("dev", None, None), P("dev", None), P("dev", None, None))
    return jax.shard_map(
        per_device, mesh=mesh, in_specs=in_specs, out_specs=out_specs, check_vma=False
    )
```
